32 devices in a mesh: curve: 8 (over z, x), grp: 4 (over y, core).
Axes of the slice: x: 2, y: 2, z: 4, core: 2. Of those that a mesh axis runs over, the one named last changes fastest.
Arguments:
- state: float32 [2, 512, 4, 12288], P(None, None, 'grp', 'curve'), may hold values from -6 to 6
- coef: float32 [512, 4, 12288], P(None, 'grp', 'curve'), may hold values from 0.2 to 4
- counts: int32 [4, 8], P('grp', 'curve'), may hold values from 512 to 1536, as said below
Outputs:
- smoothed: float32 [512, 4, 8192], P(None, 'grp', 'curve')
The draws below stay inside these ranges and needn't reach their ends.
Inputs may be any that keep to these rules, and one draw needn't show every extreme that they name: `counts`: each rank's count is 1024 plus the drift at its own end minus the drift at the end of the rank before it; drifts lie in -256 to 256, are zero before the first rank and at the last rank, so the curve holds 8192 blocks; in every curve one rank holds exactly 1536 blocks.
All inputs are finite; a program needn't handle non-finite values.
Results may differ from the reference program's by a relative error of at most 0.00002.
Values sent between devices are 32-bit elements; how exact they have to be, the bound alone decides.
No kernel may reach another device: no remote copies, remote signals or barrier semaphores. Data moves between devices by JAX's collectives and lax.ppermute only.
A program may use at most 128 MiB of HBM per device.

```python
import math
import jax
import jax.numpy as jnp

AVG = 1024
HALF = 256
CAP = 1536
SWEEPS = 2
N_CURVE = 8
N_GRP = 4


def draw_counts(key, part):
    key_walk, key_peak = jax.random.split(jax.random.fold_in(key, 11))
    drift = jax.random.randint(key_walk, (N_GRP, N_CURVE), -HALF, HALF + 1)
    peak = jax.random.randint(key_peak, (N_GRP, 1), 1, N_CURVE - 1)
    column = jnp.arange(N_CURVE, dtype=jnp.int32)[None, :]
    drift = jnp.where(column == peak, HALF, jnp.where(column == peak - 1, -HALF, drift))
    drift = jnp.where(column == N_CURVE - 1, 0, drift)
    before = jnp.concatenate([jnp.zeros((N_GRP, 1), jnp.int32), drift[:, :-1]], axis=1)
    return (AVG + drift - before).astype(jnp.int32)


def block_scale(stream_key, extent, pieces, smallest, high):
    loudness, own = 1.0, jax.random.fold_in(stream_key, 6)
    for axis_at, shards_of in pieces:
        draws = jnp.exp(jax.random.uniform(jax.random.fold_in(own, axis_at), (shards_of,), jnp.float32, smallest / len(pieces), high / len(pieces)))
        loudness = loudness * jnp.repeat(draws, extent[axis_at] // shards_of).reshape([-1 if axis == axis_at else 1 for axis in range(len(extent))])
    return loudness


def gaussian(key, dims, scale, limit, pieces=(), held_as=jnp.bfloat16):
    level = block_scale(key, dims, pieces, -0.22, 0.18) if pieces else 1.0
    values = jax.random.normal(key, dims, jnp.float32) * scale * level
    return jnp.minimum(jnp.maximum(values, -limit), limit).astype(held_as)


def setup_inputs(seed: int = 0) -> dict:
    key_list = jax.random.split(jax.random.key(seed), 4)
    return {
        "state": gaussian(key_list[0], (2, 512, N_GRP, N_CURVE * CAP), 1.0, 6.0, ((2, 4), (3, 8)), jnp.float32),
        "coef": jnp.clip(jnp.exp(math.log(4.0) - 2.9957323 * jax.random.uniform(key_list[1], (512, N_GRP, N_CURVE * CAP), jnp.float32) ** block_scale(key_list[1], (512, N_GRP, N_CURVE * CAP), ((1, 4), (2, 8)), -0.2, 0.2)), 0.2, 4.0),
        "counts": draw_counts(jax.random.fold_in(key_list[3], 71), 0),
    }


def smooth(field, source, coef, left_block, right_block, low_face, high_face):
    xplus = jnp.concatenate([field[1:], jnp.concatenate([field[0:1, :, :, :, 1:], right_block[0:1]], axis=4)], axis=0)
    xminus = jnp.concatenate([jnp.concatenate([left_block[7:8], field[7:8, :, :, :, :-1]], axis=4), field[:-1]], axis=0)
    yplus = jnp.concatenate([field[:, 1:], high_face[:, None]], axis=1)
    yminus = jnp.concatenate([low_face[:, None], field[:, :-1]], axis=1)
    zeroes = jnp.zeros_like(field[:, :, 0:1])
    zplus = jnp.concatenate([field[:, :, 1:], zeroes], axis=2)
    zminus = jnp.concatenate([zeroes, field[:, :, :-1]], axis=2)
    total = xplus + xminus + yplus + yminus + zplus + zminus
    return (source + total) / (6.0 + coef)


def reference(state, coef, counts):
    prefix = jnp.cumsum(counts, axis=1) - counts
    blocks = N_CURVE * AVG
    target = jnp.arange(blocks, dtype=jnp.int32)
    owner = jnp.sum((prefix[:, None, :] <= target[None, :, None]).astype(jnp.int32), axis=2) - 1
    start = jnp.take_along_axis(prefix, owner, axis=1)
    source_col = (owner * CAP + target[None, :] - start).astype(jnp.int32)
    moved = jnp.take_along_axis(state, jnp.broadcast_to(source_col[None, None], (2, 512, N_GRP, blocks)), axis=3)
    moved_coef = jnp.take_along_axis(coef, jnp.broadcast_to(source_col[None], (512, N_GRP, blocks)), axis=2)
    field = moved[0].reshape(8, 8, 8, N_GRP, blocks)
    source = moved[1].reshape(8, 8, 8, N_GRP, blocks)
    cellcoef = moved_coef.reshape(8, 8, 8, N_GRP, blocks)
    edge = jnp.zeros((8, 8, 8, N_GRP, 1), jnp.float32)
    plane = jnp.zeros((8, 8, 1, blocks), jnp.float32)
    for sweep in range(SWEEPS):
        low_face = jnp.concatenate([plane, field[:, 7, :, :-1, :]], axis=2)
        high_face = jnp.concatenate([field[:, 0, :, 1:, :], plane], axis=2)
        field = smooth(field, source, cellcoef, edge, edge, low_face, high_face)
    return field.reshape(512, N_GRP, blocks)
```

```python
import jax
import jax.numpy as jnp
from jax import lax
from jax.experimental import pallas as pl
from jax.experimental.pallas import tpu as pltpu
from jax.sharding import PartitionSpec as P

AVG = 1024
HALF = 256
CAP = 1536
SWEEPS = 2

LANES = 128
OWN = CAP // LANES
ZONE = HALF // LANES
WIN = AVG // LANES
SLAB = 8 * OWN
CELLS = 512
PAD = 16
F32 = jnp.float32
ANY = pl.BlockSpec(memory_space=pl.ANY)
SMEM = pl.BlockSpec(memory_space=pltpu.SMEM)


def iota(shape, dim):
    return lax.broadcasted_iota(jnp.int32, shape, dim)


def copies(pairs, sems):
    return [pltpu.make_async_copy(a, b, sems.at[i]) for i, (a, b) in enumerate(pairs)]


def run_copies(pairs, sems):
    todo = copies(pairs, sems)
    for copy in todo:
        copy.start()
    for copy in todo:
        copy.wait()


def tail_place(held):
    first = held - HALF
    return lax.div(first, LANES), lax.rem(first, LANES)


def put_zones(load, tail, head, base, place):
    row, shift = place
    lane = iota((8, LANES), 1)
    for i in range(ZONE):
        head[pl.ds(base + i, 8, stride=ZONE), :] = load(i)
    rows = [load(jnp.minimum(row + i, OWN - 1)) for i in range(ZONE + 1)]
    back = lax.rem(LANES - shift, LANES)
    for i in range(ZONE):
        both = jnp.where(lane >= shift, rows[i], rows[i + 1])
        tail[pl.ds(base + i, 8, stride=ZONE), :] = pltpu.roll(both, back, 1)


def send_zones(tail, head, even_out, odd_out, sem, even):
    @pl.when(even)
    def _():
        run_copies([(tail, even_out), (head, odd_out)], sem)

    @pl.when(jnp.logical_not(even))
    def _():
        run_copies([(head, even_out), (tail, odd_out)], sem)


def take_zones(even_in, odd_in, tail, head, sem, even):
    @pl.when(even)
    def _():
        run_copies([(odd_in, tail), (even_in, head)], sem)

    @pl.when(jnp.logical_not(even))
    def _():
        run_copies([(even_in, tail), (odd_in, head)], sem)


def is_even(axis):
    return lax.rem(lax.axis_index(axis), 2) == 0


def up8(v):
    n = v.shape[0]
    z = lax.rem(iota(v.shape, 0), 8)
    return jnp.where(z < 7, pltpu.roll(v, n - 1, 0), 0.0)


def down8(v):
    z = lax.rem(iota(v.shape, 0), 8)
    return jnp.where(z > 0, pltpu.roll(v, 1, 0), 0.0)


def edge_rows(u_ref, s_ref, c_ref, outer, row, lane, extra_row):
    inner = 6 if outer == 7 else 1

    def at(ref, x, r):
        return ref[pl.ds(PAD + x * 8 * SLAB + r, 64, stride=OWN), :]

    u = at(u_ref, outer, row)
    side = s_ref[pl.ds(row, 64, stride=OWN), :] + at(u_ref, inner, row) + up8(u) + down8(u)
    zero = jnp.zeros((8, LANES), F32)
    side += jnp.concatenate([zero, u[:-8]], 0) + jnp.concatenate([u[8:], zero], 0)
    parts = [(u, side), (c_ref[pl.ds(row, 64, stride=OWN), :], at(u_ref, outer, extra_row))]
    back = lax.rem(LANES - lane, LANES)
    rows = []
    for pair in parts:
        square = pltpu.roll(jnp.concatenate(pair, 0), back, 1)
        rows.append(jnp.transpose(square)[0:1])
    return rows


def spread(packed):
    return jnp.transpose(jnp.broadcast_to(packed, (LANES, LANES)))


def faces_kernel(held_ref, state, coef, even_out, odd_out, u, s, c, tail, head, sem):
    held = held_ref[0, 0]
    rows = 8 * SLAB
    run_copies(
        [
            (state.at[0], u.at[pl.ds(PAD, 8 * rows)]),
            (state.at[1, pl.ds(0, rows)], s.at[0]),
            (state.at[1, pl.ds(7 * rows, rows)], s.at[1]),
            (coef.at[pl.ds(0, rows)], c.at[0]),
            (coef.at[pl.ds(7 * rows, rows)], c.at[1]),
        ],
        sem,
    )
    place = tail_place(held)
    for plane in range(2):
        for x in range(8):
            start = PAD + (x * 8 + 7 * plane) * SLAB
            load = lambda r, start=start: u[pl.ds(start + r, 8, stride=OWN), :]
            put_zones(load, tail, head, (plane * 8 + x) * 8 * ZONE, place)
    end = held - 1
    row, lane = lax.div(end, LANES), lax.rem(end, LANES)
    edge = 2 * 64 * ZONE
    blank = jnp.zeros((6, LANES), F32)
    first = edge_rows(u, s.at[0], c.at[0], 0, 0, 0, ZONE)
    head[pl.ds(edge, 8), :] = jnp.concatenate(first + [blank], 0)
    last = edge_rows(u, s.at[1], c.at[1], 7, row, lane, row - ZONE)
    tail[pl.ds(edge, 8), :] = jnp.concatenate(last + [blank], 0)
    send_zones(tail, head, even_out, odd_out, sem, is_even("curve"))


def rest_kernel(held_ref, state, coef, even_out, odd_out, u, s, c, tail, head, sem):
    run_copies(
        [(state.at[0, :, y], u.at[i]) for i, y in enumerate((1, 6))]
        + [(state.at[1, :, y], s.at[i]) for i, y in enumerate((0, 7))]
        + [(coef.at[:, y], c.at[i]) for i, y in enumerate((0, 1, 6, 7))],
        sem,
    )
    place = tail_place(held_ref[0, 0])

    def at(ref, i, x):
        return lambda r: ref[i, x, pl.ds(r, 8, stride=OWN), :]

    def both(i, x):
        return lambda r: at(u, i, x)(r) + at(s, i, x)(r)

    def body(x, carry):
        loads = [both(0, x)] + [at(c, i, x) for i in range(4)] + [both(1, x)]
        for plane, load in enumerate(loads):
            put_zones(load, tail, head, (plane * 8 + x) * 8 * ZONE, place)
        return carry

    lax.fori_loop(0, 8, body, 0)
    send_zones(tail, head, even_out, odd_out, sem, is_even("curve"))


def sweep_kernel(held_ref, state, coef, even_in, odd_in, pack, even_out, odd_out, u, s, c, v, w, edges, tail, head, sem):
    held = held_ref[0, 0]
    even = is_even("curve")
    rank, ranks = lax.axis_index("curve"), lax.axis_size("curve")
    rows = CELLS * OWN
    edge = 2 * 64 * ZONE
    run_copies(
        [
            (state.at[0], u.at[pl.ds(PAD, rows)]),
            (state.at[1], s),
            (coef, c),
        ],
        sem,
    )
    take_zones(
        even_in.at[pl.ds(edge, 8)], odd_in.at[pl.ds(edge, 8)], edges.at[0], edges.at[1], sem, even
    )
    row96 = iota((SLAB, LANES), 0)
    lane96 = iota((SLAB, LANES), 1)
    slot = lax.rem(row96, OWN) * LANES + lane96
    zlast, zfirst = row96 >= SLAB - OWN, row96 < OWN
    last_lane, first_lane = lane96 == LANES - 1, lane96 == 0
    starts = slot == 0
    ends = slot == held - 1

    def zsum(ref, b):
        up = jnp.where(zlast, 0.0, ref[pl.ds(b + OWN, SLAB), :])
        down = jnp.where(zfirst, 0.0, ref[pl.ds(b - OWN, SLAB), :])
        return up + down

    step = 8 * SLAB

    def left(ref, b):
        both = jnp.where(last_lane, ref[pl.ds(b - 1, SLAB), :], ref[pl.ds(b, SLAB), :])
        return jnp.where(starts, 0.0, pltpu.roll(both, 1, 1))

    def right(ref, b):
        both = jnp.where(first_lane, ref[pl.ds(b + 1, SLAB), :], ref[pl.ds(b, SLAB), :])
        return jnp.where(ends, 0.0, pltpu.roll(both, LANES - 1, 1))

    def xsum(ref, b, kind):
        if kind == 0:
            return left(ref, b + 7 * step) + ref[pl.ds(b + step, SLAB), :]
        if kind == 2:
            return ref[pl.ds(b - step, SLAB), :] + right(ref, b - 7 * step)
        return ref[pl.ds(b - step, SLAB), :] + ref[pl.ds(b + step, SLAB), :]

    def first(x, kind):
        def body(y, carry):
            b = (x * 8 + y) * SLAB
            if not isinstance(b, int):
                b = pl.multiple_of(b, 8)
            p = b + PAD
            total = s[pl.ds(b, SLAB), :] + zsum(u, p) + xsum(u, p, kind)
            total += u[pl.ds(p - SLAB, SLAB), :] + u[pl.ds(p + SLAB, SLAB), :]
            v[pl.ds(p, SLAB), :] = total / (6.0 + c[pl.ds(b, SLAB), :])
            return carry

        lax.fori_loop(1, 7, body, 0)

    each_x(first)

    end_row, end_lane = lax.div(held - 1, LANES), lax.rem(held - 1, LANES)
    lane = iota((64, LANES), 1)
    mine = []
    for side, x, at_row, at_lane, there in (
        (0, 0, 0, 0, rank > 0),
        (1, 7, end_row, end_lane, rank < ranks - 1),
    ):
        a = spread(edges[side, 0:1, :])
        b = spread(edges[side, 1:2, :])
        place = pl.ds(PAD + x * step + at_row, 64, stride=OWN)
        plain = pl.ds(x * step + at_row, 64, stride=OWN)
        hit = lane == at_lane
        cell = c[plain, :]
        v[place, :] = v[place, :] + jnp.where(hit, a[:64] / (6.0 + cell), 0.0)
        beyond = (a[64:] + u[place, :]) / (6.0 + b[:64])
        mine.append(jnp.where(jnp.logical_and(hit, there), beyond, 0.0))

    def second(x, kind):
        def at(y):
            b = (x * 8 + y) * SLAB
            if not isinstance(b, int):
                b = pl.multiple_of(b, 8)
            return b, b + PAD

        def put(y, value):
            o = (y * 8 + x) * SLAB
            if not isinstance(o, int):
                o = pl.multiple_of(o, 8)
            w[pl.ds(o, SLAB), :] = value

        for y, inner in ((0, 1), (7, 6)):
            put(y, s[pl.ds(at(y)[0], SLAB), :] + v[pl.ds(at(inner)[1], SLAB), :])
        for y, inner in ((1, 2), (6, 5)):
            b, p = at(y)
            total = s[pl.ds(b, SLAB), :] + zsum(v, p) + xsum(v, p, kind)
            put(y, total + v[pl.ds(at(inner)[1], SLAB), :])

        def body(y, carry):
            b = (x * 8 + y) * SLAB
            b = b if isinstance(b, int) else pl.multiple_of(b, 8)
            p = b + PAD
            total = s[pl.ds(b, SLAB), :] + zsum(v, p) + xsum(v, p, kind)
            total += v[pl.ds(p - SLAB, SLAB), :] + v[pl.ds(p + SLAB, SLAB), :]
            o = pl.multiple_of((y * 8 + x) * SLAB, 8)
            w[pl.ds(o, SLAB), :] = total / (6.0 + c[pl.ds(b, SLAB), :])
            return carry

        lax.fori_loop(2, 6, body, 0)

    each_x(second)

    for side, x, at_row in ((0, 0, 0), (1, 7, end_row)):
        for y in range(1, 7):
            o = pl.ds((y * 8 + x) * SLAB + at_row, 8, stride=OWN)
            more = mine[side][8 * y : 8 * y + 8]
            if 2 <= y <= 5:
                more = more / (6.0 + c[pl.ds((x * 8 + y) * SLAB + at_row, 8, stride=OWN), :])
            w[o, :] = w[o, :] + more

    place = tail_place(held)

    def body(i, carry):
        load = lambda r: w[pl.ds(i * SLAB + r, 8, stride=OWN), :]
        put_zones(load, tail, head, pl.multiple_of(i * 8 * ZONE, 8), place)
        return carry

    lax.fori_loop(0, 64, body, 0)
    save = pltpu.make_async_copy(w, pack, sem.at[7])
    save.start()
    send_zones(tail, head, even_out, odd_out, sem, even)
    save.wait()


class Window:
    def __init__(self, before, after):
        self.lane = iota((WIN, LANES), 1)
        self.row = iota((WIN, LANES), 0)
        j = self.row * LANES + self.lane
        down = lambda n: lax.shift_right_arithmetic(n, 7)
        self.own_row = down(-before)
        self.own_lane = jnp.bitwise_and(-before, LANES - 1)
        self.head_row = down(-AVG - after)
        self.head_lane = jnp.bitwise_and(-AVG - after, LANES - 1)
        self.tail_row = self.own_row + ZONE
        self.from_tail = j < before
        self.from_head = j >= AVG + after

    def take(self, ref, start, row, shift):
        a = ref[pl.ds(start + row, WIN), :]
        b = ref[pl.ds(start + row + 1, WIN), :]
        return pltpu.roll(
            jnp.where(self.lane >= shift, a, b), jnp.bitwise_and(LANES - shift, LANES - 1), 1
        )

    def __call__(self, own, own_at, tail, tail_at, head, head_at):
        mine = self.take(own, own_at, self.own_row, self.own_lane)
        prev = self.take(tail, tail_at, self.tail_row, self.own_lane)
        after = self.take(head, head_at, self.head_row, self.head_lane)
        return jnp.where(self.from_tail, prev, jnp.where(self.from_head, after, mine))


def drifts(held_ref, before_ref):
    rank = lax.axis_index("curve")
    before = before_ref[0, 0] - rank * AVG
    return before, before + held_ref[0, 0] - AVG


def face_planes(ref, state_or_coef, planes, where):
    size = 8 * SLAB
    return [
        (state_or_coef.at[:, y], ref.at[pl.ds(PAD + i * size, size)].reshape(8, SLAB, LANES))
        for y, i in zip(planes, where)
    ]


def send_faces(low, high, even_out, odd_out, sem):
    even = is_even("grp")

    @pl.when(even)
    def _():
        run_copies([(high, even_out), (low, odd_out)], sem)

    @pl.when(jnp.logical_not(even))
    def _():
        run_copies([(low, even_out), (high, odd_out)], sem)


def take_faces(even_in, odd_in, low, high, sem):
    even = is_even("grp")

    @pl.when(even)
    def _():
        run_copies([(odd_in, low), (even_in, high)], sem)

    @pl.when(jnp.logical_not(even))
    def _():
        run_copies([(even_in, low), (odd_in, high)], sem)


def align_kernel(
    held_ref, before_ref, state, even_in, odd_in,
    even_out, odd_out, faces, sides,
    own, tail, head, edges, sem,
):
    before, after = drifts(held_ref, before_ref)
    even = is_even("curve")
    edge = 2 * 64 * ZONE
    run_copies(face_planes(own, state.at[0], (0, 7), (0, 1)), sem)
    zone = pl.ds(PAD, edge)
    take_zones(
        even_in.at[pl.ds(0, edge)], odd_in.at[pl.ds(0, edge)], tail.at[zone], head.at[zone], sem, even
    )
    packed = pl.ds(edge, 8)
    take_zones(even_in.at[packed], odd_in.at[packed], edges.at[0], edges.at[1], sem, even)
    here = Window(before, after)

    def body(i, carry):
        at = PAD + i * OWN
        zat = PAD + i * ZONE
        faces[pl.ds(pl.multiple_of(i * WIN, 8), WIN), :] = here(own, at, tail, zat, head, zat)
        return carry

    lax.fori_loop(0, 128, body, 0)
    lower = Window(before + 1, after + 1)
    upper = Window(before - 1, after - 1)
    j = here.row * LANES + here.lane
    for side, window, x, lost in (
        (0, lower, 7, jnp.logical_and(j == 0, before == HALF)),
        (1, upper, 0, jnp.logical_and(j == AVG - 1, after == -HALF)),
    ):
        beyond = spread(edges[side, 1:2, :])[64:]
        for plane in range(2):
            for z in range(8):
                i = (plane * 8 + x) * 8 + z
                at = PAD + i * OWN
                zat = PAD + i * ZONE
                value = window(own, at, tail, zat, head, zat)
                y = 56 * plane + z
                value = jnp.where(lost, beyond[y : y + 1], value)
                sides[pl.ds(((side * 2 + plane) * 8 + z) * WIN, WIN), :] = value
    half = 64 * WIN
    send_faces(faces.at[pl.ds(0, half)], faces.at[pl.ds(half, half)], even_out, odd_out, sem)


def each_x(run):
    run(0, 0)

    def mid(x, carry):
        run(x, 1)
        return carry

    lax.fori_loop(1, 7, mid, 0)
    run(7, 2)


def cell_rows(plane, x, z):
    at = ((plane * 8 + x) * 8 + z) * WIN
    return pl.ds(at if isinstance(at, int) else pl.multiple_of(at, 8), WIN)


def face_kernel(
    held_ref, before_ref, state, coef, even_in, odd_in, even_face, odd_face, faces, sides,
    even_out, odd_out, even_end, odd_end, new, below, inner,
    own, tail, head, near, q, ends, sem,
):
    before, after = drifts(held_ref, before_ref)
    even = is_even("curve")
    size = 6 * 64 * ZONE
    half = 64 * WIN
    run_copies(
        face_planes(own, state.at[0], (1, 6), (0, 5))
        + face_planes(own, coef, (0, 1, 6, 7), (1, 2, 3, 4))
        + face_planes(own, state.at[1], (0, 7), (6, 7)),
        sem,
    )
    zone = pl.ds(PAD, size)
    take_zones(even_in, odd_in, tail.at[zone], head.at[zone], sem, even)
    take_faces(even_face, odd_face, near.at[pl.ds(0, half)], near.at[pl.ds(half, half)], sem)
    for to, more in ((0, 6), (5, 7)):
        for x in range(8):
            a = pl.ds(PAD + (to * 8 + x) * SLAB, SLAB)
            b = pl.ds(PAD + (more * 8 + x) * SLAB, SLAB)
            own[a, :] = own[a, :] + own[b, :]
    here = Window(before, after)

    def body(i, carry):
        for plane, ref, to, add in (
            (0, q, 0, 0.0),
            (5, q, 1, 0.0),
            (1, below, 0, 6.0),
            (4, below, 1, 6.0),
            (2, inner, 0, 6.0),
            (3, inner, 1, 6.0),
        ):
            at = PAD + (plane * 64 + i) * OWN
            zat = PAD + (plane * 64 + i) * ZONE
            value = here(own, at, tail, zat, head, zat)
            ref[pl.ds(pl.multiple_of((to * 64 + i) * WIN, 8), WIN), :] = value + add
        return carry

    lax.fori_loop(0, 64, body, 0)

    def run(x, kind):
        for plane in range(2):
            for z in range(8):
                here = cell_rows(plane, x, z)
                total = q[here, :] + near[here, :]
                if kind == 0:
                    total += sides[pl.ds((plane * 8 + z) * WIN, WIN), :]
                else:
                    total += faces[cell_rows(plane, x - 1, z), :]
                if kind == 2:
                    total += sides[pl.ds(((2 + plane) * 8 + z) * WIN, WIN), :]
                else:
                    total += faces[cell_rows(plane, x + 1, z), :]
                if z > 0:
                    total += faces[cell_rows(plane, x, z - 1), :]
                if z < 7:
                    total += faces[cell_rows(plane, x, z + 1), :]
                new[here, :] = total / below[here, :]

    each_x(run)
    for plane in range(2):
        for z in range(8):
            i = plane * 8 + z
            ends[0, i : i + 1, :] = new[pl.ds(((plane * 8 + 7) * 8 + z) * WIN + WIN - 1, 1), :]
            ends[1, i : i + 1, :] = new[pl.ds((plane * 64 + z) * WIN, 1), :]
    send_faces(new.at[pl.ds(0, half)], new.at[pl.ds(half, half)], even_out, odd_out, sem)
    send_zones(ends.at[0], ends.at[1], even_end, odd_end, sem, even)


def last_kernel(
    held_ref, before_ref, pack, even_in, odd_in, even_face, odd_face, even_end, odd_end,
    new, below, inner,
    out,
    own, tail, head, near, ends, sem,
):
    before, after = drifts(held_ref, before_ref)
    even = is_even("curve")
    size = 8 * 64 * ZONE
    half = 64 * WIN
    fetch = pltpu.make_async_copy(pack, own.at[pl.ds(PAD, CELLS * OWN)], sem.at[7])
    fetch.start()
    zone = pl.ds(PAD, size)
    take_zones(even_in, odd_in, tail.at[zone], head.at[zone], sem, even)
    take_zones(even_end, odd_end, ends.at[0], ends.at[1], sem, even)
    take_faces(even_face, odd_face, near.at[pl.ds(0, half)], near.at[pl.ds(half, half)], sem)
    fetch.wait()
    here = Window(before, after)
    lane, row = here.lane, here.row

    def get(y, x, z):
        i = (y * 8 + x) * 8 + z
        return here(own, PAD + i * OWN, tail, PAD + i * ZONE, head, PAD + i * ZONE)

    def put(x, y, z, value):
        at = ((x * 8 + y) * 8 + z) * WIN
        out[pl.ds(at if isinstance(at, int) else pl.multiple_of(at, 8), WIN), :] = value

    def left(plane, z):
        v = pltpu.roll(new[cell_rows(plane, 7, z), :], 1, 1)
        i = plane * 8 + z
        edge = pltpu.roll(jnp.broadcast_to(ends[0, i : i + 1, :], (WIN, LANES)), 1, 1)
        return jnp.where(lane == 0, jnp.where(row == 0, edge, pltpu.roll(v, 1, 0)), v)

    def right(plane, z):
        v = pltpu.roll(new[cell_rows(plane, 0, z), :], LANES - 1, 1)
        i = plane * 8 + z
        edge = pltpu.roll(jnp.broadcast_to(ends[1, i : i + 1, :], (WIN, LANES)), LANES - 1, 1)
        next_row = jnp.where(row == WIN - 1, edge, pltpu.roll(v, WIN - 1, 0))
        return jnp.where(lane == LANES - 1, next_row, v)

    def run(x, kind):
        for plane, y in ((0, 0), (1, 7)):
            for z in range(8):
                cell = cell_rows(plane, x, z)
                total = get(y, x, z) + near[cell, :]
                total += left(plane, z) if kind == 0 else new[cell_rows(plane, x - 1, z), :]
                total += right(plane, z) if kind == 2 else new[cell_rows(plane, x + 1, z), :]
                if z > 0:
                    total += new[cell_rows(plane, x, z - 1), :]
                if z < 7:
                    total += new[cell_rows(plane, x, z + 1), :]
                put(x, y, z, total / below[cell, :])
        for plane, y in ((0, 1), (1, 6)):
            for z in range(8):
                cell = cell_rows(plane, x, z)
                put(x, y, z, (get(y, x, z) + new[cell, :]) / inner[cell, :])
        for y in range(2, 6):
            for z in range(8):
                put(x, y, z, get(y, x, z))

    each_x(run)


def swapped(value, axis, first):
    count = lax.axis_size(axis)
    pairs = [(i, i + 1) for i in range(first, count - 1, 2)]
    return lax.ppermute(value, axis, pairs + [(b, a) for a, b in pairs])


def swaps(values, axis):
    return tuple(swapped(value, axis, first) for first, value in enumerate(values))


def held_before(counts):
    rank, count = lax.axis_index("curve"), lax.axis_size("curve")
    total, before, bit = counts, jnp.zeros_like(counts), 1
    while bit < count:
        other = lax.ppermute(total, "curve", [(i, i ^ bit) for i in range(count) if i ^ bit < count])
        before += jnp.where(jnp.bitwise_and(rank, bit) != 0, other, 0)
        total += other
        bit *= 2
    return before


def array(*shape):
    return jax.ShapeDtypeStruct(shape, F32)


def call(kernel, outs, ins, scratch, sems=8, vmem_ins=(), vmem_outs=None, scalars=1, cost=4000):
    vmem = pl.BlockSpec(memory_space=pltpu.VMEM)
    specs = [SMEM] * scalars
    specs += [vmem if i in vmem_ins else ANY for i in range(scalars, len(ins))]
    return pl.pallas_call(
        kernel,
        out_shape=outs,
        in_specs=specs,
        out_specs=[vmem if vmem_outs and i in vmem_outs else ANY for i in range(len(outs))],
        scratch_shapes=[pltpu.VMEM(shape, F32) for shape in scratch] + [pltpu.SemaphoreType.DMA((sems,))],
        compiler_params=pltpu.CompilerParams(vmem_limit_bytes=40 * 2**20),
        cost_estimate=pl.CostEstimate(flops=cost * 4000, bytes_accessed=cost * 1000, transcendentals=0),
    )(*ins)


def local(state, coef, counts):
    state3 = state.reshape(2, CELLS * OWN, LANES)
    coef2 = coef.reshape(CELLS * OWN, LANES)
    state5 = state.reshape(2, 8, 8, SLAB, LANES)
    coef4 = coef.reshape(8, 8, SLAB, LANES)
    rows = CELLS * OWN
    step = 8 * SLAB
    zone = 64 * ZONE
    win = 64 * WIN

    before = held_before(counts)
    message = (2 * zone + 8, LANES)
    faces_out = call(
        faces_kernel,
        [array(*message)] * 2,
        (counts, state3, coef2),
        [(rows + 2 * PAD, LANES), (2, step, LANES), (2, step, LANES), message, message],
    )
    faces_in = swaps(faces_out, "curve")
    message = (6 * zone, LANES)
    rest_out = call(
        rest_kernel,
        [array(*message)] * 2,
        (counts, state5, coef4),
        [(2, 8, SLAB, LANES), (2, 8, SLAB, LANES), (4, 8, SLAB, LANES), message, message],
    )
    rest_in = swaps(rest_out, "curve")
    message = (8 * zone, LANES)
    pack, *sweep_out = call(
        sweep_kernel,
        [array(rows, LANES)] + [array(*message)] * 2,
        (counts, state3, coef2, *faces_in),
        [
            (rows + 2 * PAD, LANES), (rows, LANES), (rows, LANES), (rows + 2 * PAD, LANES),
            (rows, LANES), (2, 8, LANES), message, message,
        ],
    )
    sweep_in = swaps(sweep_out, "curve")
    *near_out, faces, sides = call(
        align_kernel,
        [array(win, LANES)] * 2 + [array(2 * win, LANES), array(32 * WIN, LANES)],
        (counts, before, state5, *faces_in),
        [
            (2 * step + 2 * PAD, LANES), (2 * zone + 2 * PAD, LANES), (2 * zone + 2 * PAD, LANES),
            (2, 8, LANES),
        ],
        vmem_outs=(2, 3),
        scalars=2,
    )
    near_in = swaps(near_out, "grp")
    near_a, near_b, end_a, end_b, new, below, inner = call(
        face_kernel,
        [array(win, LANES)] * 2 + [array(16, LANES)] * 2 + [array(2 * win, LANES)] * 3,
        (counts, before, state5, coef4, *rest_in, *near_in, faces, sides),
        [
            (8 * step + 2 * PAD, LANES), (6 * zone + 2 * PAD, LANES), (6 * zone + 2 * PAD, LANES),
            (2 * win, LANES), (2 * win, LANES), (2, 16, LANES),
        ],
        vmem_ins=(8, 9),
        vmem_outs=(4, 5, 6),
        scalars=2,
    )
    near_in = swaps((near_a, near_b), "grp")
    end_in = swaps((end_a, end_b), "curve")
    (out,) = call(
        last_kernel,
        [array(CELLS * WIN, LANES)],
        (counts, before, pack, *sweep_in, *near_in, *end_in, new, below, inner),
        [
            (rows + 2 * PAD, LANES), (8 * zone + 2 * PAD, LANES), (8 * zone + 2 * PAD, LANES),
            (2 * win, LANES), (2, 16, LANES),
        ],
        vmem_ins=(9, 10, 11),
        vmem_outs=(0,),
        scalars=2,
    )
    return out.reshape(CELLS, 1, AVG)


def solution(mesh):
    placed = (P(None, None, "grp", "curve"), P(None, "grp", "curve"), P("grp", "curve"))
    return jax.shard_map(
        local, mesh=mesh, in_specs=placed, out_specs=P(None, "grp", "curve"), check_vma=False
    )
```

```python
import jax
import jax.numpy as jnp
from jax import lax
from jax.experimental import pallas as pl
from jax.experimental.pallas import tpu as pltpu
from jax.sharding import PartitionSpec as P


AVG = 1024
HALF = 256
CAP = 1536

LANES = 128
OWN = CAP // LANES
ZONE = HALF // LANES
WIN = AVG // LANES
SLAB = 8 * OWN
CELLS = 512
PAD = 16
F32 = jnp.float32
ANY = pl.BlockSpec(memory_space=pl.ANY)
HBM = pl.BlockSpec(memory_space=pltpu.HBM)
SMEM = pl.BlockSpec(memory_space=pltpu.SMEM)


def iota(shape, dim):
    return lax.broadcasted_iota(jnp.int32, shape, dim)


def copies(pairs, sems):
    return [pltpu.make_async_copy(a, b, sems.at[i]) for i, (a, b) in enumerate(pairs)]


def run_copies(pairs, sems):
    todo = copies(pairs, sems)
    for copy in todo:
        copy.start()
    for copy in todo:
        copy.wait()


def tail_place(held):
    first = held - HALF
    return lax.div(first, LANES), lax.rem(first, LANES)


def put_zones(load, tail, head, base, place):
    row, shift = place
    lane = iota((8, LANES), 1)
    for i in range(ZONE):
        head[pl.ds(base + i, 8, stride=ZONE), :] = load(i)
    rows = [load(jnp.minimum(row + i, OWN - 1)) for i in range(ZONE + 1)]
    back = lax.rem(LANES - shift, LANES)
    for i in range(ZONE):
        both = jnp.where(lane >= shift, rows[i], rows[i + 1])
        tail[pl.ds(base + i, 8, stride=ZONE), :] = pltpu.roll(both, back, 1)


def send_zones(tail, head, even_out, odd_out, sem, even):
    @pl.when(even)
    def _():
        run_copies([(tail, even_out), (head, odd_out)], sem)

    @pl.when(jnp.logical_not(even))
    def _():
        run_copies([(head, even_out), (tail, odd_out)], sem)


def take_zones(even_in, odd_in, tail, head, sem, even):
    @pl.when(even)
    def _():
        run_copies([(odd_in, tail), (even_in, head)], sem)

    @pl.when(jnp.logical_not(even))
    def _():
        run_copies([(even_in, tail), (odd_in, head)], sem)


def is_even(axis):
    return lax.rem(lax.axis_index(axis), 2) == 0


def up8(v):
    n = v.shape[0]
    z = lax.rem(iota(v.shape, 0), 8)
    return jnp.where(z < 7, pltpu.roll(v, n - 1, 0), 0.0)


def down8(v):
    z = lax.rem(iota(v.shape, 0), 8)
    return jnp.where(z > 0, pltpu.roll(v, 1, 0), 0.0)


def edge_rows(u_ref, s_ref, c_ref, outer, row, lane, extra_row):
    inner = 6 if outer == 7 else 1

    def at(ref, x, r):
        return ref[pl.ds(x * 8 * SLAB + r, 64, stride=OWN), :]

    u = at(u_ref, outer, row)
    side = at(s_ref, outer, row) + at(u_ref, inner, row) + up8(u) + down8(u)
    zero = jnp.zeros((8, LANES), F32)
    side += jnp.concatenate([zero, u[:-8]], 0) + jnp.concatenate([u[8:], zero], 0)
    parts = [(u, side), (at(c_ref, outer, row), at(u_ref, outer, extra_row))]
    back = lax.rem(LANES - lane, LANES)
    rows = []
    for pair in parts:
        square = pltpu.roll(jnp.concatenate(pair, 0), back, 1)
        rows.append(jnp.transpose(square)[0:1])
    return rows


def spread(packed):
    return jnp.transpose(jnp.broadcast_to(packed, (LANES, LANES)))


def front_kernel(
    held_ref, _, state, coef,
    even_out, odd_out, even_rest, odd_rest,
    tail, head, tail_rest, head_rest, sem,
):
    held = held_ref[0, 0]
    rows = CELLS * OWN
    u, c = state, coef
    s = state.at[pl.ds(rows, rows)]
    place = tail_place(held)
    even = is_even("curve")

    def at(ref, x, y):
        start = (x * 8 + y) * SLAB
        return lambda r: ref[pl.ds(start + r, 8, stride=OWN), :]

    def both(x, y, inner):
        return lambda r: at(u, x, inner)(r) + at(s, x, y)(r)

    for plane in range(2):
        for x in range(8):
            put_zones(at(u, x, 7 * plane), tail, head, (plane * 8 + x) * 8 * ZONE, place)
    end = held - 1
    row, lane = lax.div(end, LANES), lax.rem(end, LANES)
    edge = 2 * 64 * ZONE
    blank = jnp.zeros((6, LANES), F32)
    first = edge_rows(u, s, c, 0, 0, 0, ZONE)
    head[pl.ds(edge, 8), :] = jnp.concatenate(first + [blank], 0)
    last = edge_rows(u, s, c, 7, row, lane, row - ZONE)
    tail[pl.ds(edge, 8), :] = jnp.concatenate(last + [blank], 0)
    for x in range(8):
        loads = [both(x, 0, 1)] + [at(c, x, y) for y in (0, 1, 6, 7)] + [both(x, 7, 6)]
        for plane, load in enumerate(loads):
            put_zones(load, tail_rest, head_rest, (plane * 8 + x) * 8 * ZONE, place)
    for flag, a, b, ra, rb in (
        (even, tail, head, tail_rest, head_rest),
        (jnp.logical_not(even), head, tail, head_rest, tail_rest),
    ):
        @pl.when(flag)
        def _():
            run_copies([(a, even_out), (b, odd_out), (ra, even_rest), (rb, odd_rest)], sem)


def sweep_kernel(
    held_ref, _, state, coef, even_in, odd_in,
    front, pack, even_out, odd_out,
    v, edges, tail, head, sem,
):
    held = held_ref[0, 0]
    even = is_even("curve")
    rank, ranks = lax.axis_index("curve"), lax.axis_size("curve")
    edge = 2 * 64 * ZONE
    packed = pl.ds(edge, 8)
    u, c = state, coef
    s = state.at[pl.ds(CELLS * OWN, CELLS * OWN)]
    w = pack.at[pl.ds(PAD, CELLS * OWN)]
    take_zones(even_in.at[packed], odd_in.at[packed], edges.at[0], edges.at[1], sem, even)
    row96 = iota((SLAB, LANES), 0)
    lane96 = iota((SLAB, LANES), 1)
    slot = lax.rem(row96, OWN) * LANES + lane96
    zlast, zfirst = row96 >= SLAB - OWN, row96 < OWN
    last_lane, first_lane = lane96 == LANES - 1, lane96 == 0
    starts = slot == 0
    ends = slot == held - 1

    def zsum(ref, b):
        up = jnp.where(zlast, 0.0, ref[pl.ds(b + OWN, SLAB), :])
        down = jnp.where(zfirst, 0.0, ref[pl.ds(b - OWN, SLAB), :])
        return up + down

    step = 8 * SLAB

    def left(ref, b):
        both = jnp.where(last_lane, ref[pl.ds(b - 1, SLAB), :], ref[pl.ds(b, SLAB), :])
        return jnp.where(starts, 0.0, pltpu.roll(both, 1, 1))

    def right(ref, b):
        both = jnp.where(first_lane, ref[pl.ds(b + 1, SLAB), :], ref[pl.ds(b, SLAB), :])
        return jnp.where(ends, 0.0, pltpu.roll(both, LANES - 1, 1))

    def xsum(ref, b, kind):
        if kind == 0:
            return left(ref, b + 7 * step) + ref[pl.ds(b + step, SLAB), :]
        if kind == 2:
            return ref[pl.ds(b - step, SLAB), :] + right(ref, b - 7 * step)
        return ref[pl.ds(b - step, SLAB), :] + ref[pl.ds(b + step, SLAB), :]

    def first(x, kind):
        def body(y, carry):
            b = (x * 8 + y) * SLAB
            if not isinstance(b, int):
                b = pl.multiple_of(b, 8)
            total = s[pl.ds(b, SLAB), :] + zsum(u, b) + xsum(u, b, kind)
            total += u[pl.ds(b - SLAB, SLAB), :] + u[pl.ds(b + SLAB, SLAB), :]
            v[pl.ds(b + PAD, SLAB), :] = total / (6.0 + c[pl.ds(b, SLAB), :])
            return carry

        lax.fori_loop(1, 7, body, 0)

    each_x(first)

    end_row, end_lane = lax.div(held - 1, LANES), lax.rem(held - 1, LANES)
    lane = iota((64, LANES), 1)
    mine = []
    for side, x, at_row, at_lane, there in (
        (0, 0, 0, 0, rank > 0),
        (1, 7, end_row, end_lane, rank < ranks - 1),
    ):
        a = spread(edges[side, 0:1, :])
        b = spread(edges[side, 1:2, :])
        place = pl.ds(PAD + x * step + at_row, 64, stride=OWN)
        plain = pl.ds(x * step + at_row, 64, stride=OWN)
        hit = lane == at_lane
        cell = c[plain, :]
        v[place, :] = v[place, :] + jnp.where(hit, a[:64] / (6.0 + cell), 0.0)
        beyond = (a[64:] + u[plain, :]) / (6.0 + b[:64])
        mine.append(jnp.where(jnp.logical_and(hit, there), beyond, 0.0))

    def second(x, kind):
        def at(y):
            b = (x * 8 + y) * SLAB
            if not isinstance(b, int):
                b = pl.multiple_of(b, 8)
            return b, b + PAD

        def put(y, value):
            o = (y * 8 + x) * SLAB
            if not isinstance(o, int):
                o = pl.multiple_of(o, 8)
            w[pl.ds(o, SLAB), :] = value

        for y, inner in ((0, 1), (7, 6)):
            put(y, s[pl.ds(at(y)[0], SLAB), :] + v[pl.ds(at(inner)[1], SLAB), :])
        for y, inner in ((1, 2), (6, 5)):
            b, p = at(y)
            total = s[pl.ds(b, SLAB), :] + zsum(v, p) + xsum(v, p, kind)
            put(y, total + v[pl.ds(at(inner)[1], SLAB), :])

        def body(y, carry):
            b = (x * 8 + y) * SLAB
            b = b if isinstance(b, int) else pl.multiple_of(b, 8)
            p = b + PAD
            total = s[pl.ds(b, SLAB), :] + zsum(v, p) + xsum(v, p, kind)
            total += v[pl.ds(p - SLAB, SLAB), :] + v[pl.ds(p + SLAB, SLAB), :]
            o = pl.multiple_of((y * 8 + x) * SLAB, 8)
            w[pl.ds(o, SLAB), :] = total / (6.0 + c[pl.ds(b, SLAB), :])
            return carry

        lax.fori_loop(2, 6, body, 0)

    each_x(second)

    for side, x, at_row in ((0, 0, 0), (1, 7, end_row)):
        for y in range(1, 7):
            o = pl.ds((y * 8 + x) * SLAB + at_row, 8, stride=OWN)
            more = mine[side][8 * y : 8 * y + 8]
            if 2 <= y <= 5:
                more = more / (6.0 + c[pl.ds((x * 8 + y) * SLAB + at_row, 8, stride=OWN), :])
            w[o, :] = w[o, :] + more

    place = tail_place(held)

    def body(i, carry):
        for k in range(8):
            at = pl.multiple_of((i * 8 + k) * SLAB, 8)
            load = lambda r, at=at: w[pl.ds(at + r, 8, stride=OWN), :]
            put_zones(load, tail, head, pl.multiple_of((i * 8 + k) * 8 * ZONE, 8), place)
        return carry

    lax.fori_loop(0, 8, body, 0)

    def keep(x, carry):
        def slab(ref, y):
            return ref[pl.ds(pl.multiple_of((x * 8 + y) * SLAB, 8), SLAB), :]

        for plane, value in enumerate(
            (
                slab(u, 0), slab(u, 7), slab(s, 0) + slab(u, 1), slab(c, 0),
                slab(c, 1), slab(c, 6), slab(c, 7), slab(s, 7) + slab(u, 6),
            )
        ):
            front[pl.ds(pl.multiple_of(PAD + (plane * 8 + x) * SLAB, 8), SLAB), :] = value
        return carry

    lax.fori_loop(0, 8, keep, 0)
    send_zones(tail, head, even_out, odd_out, sem, even)


class Window:
    def __init__(self, before, after):
        self.lane = iota((WIN, LANES), 1)
        self.row = iota((WIN, LANES), 0)
        j = self.row * LANES + self.lane
        down = lambda n: lax.shift_right_arithmetic(n, 7)
        self.own_row = down(-before)
        self.own_lane = jnp.bitwise_and(-before, LANES - 1)
        self.head_row = down(-AVG - after)
        self.head_lane = jnp.bitwise_and(-AVG - after, LANES - 1)
        self.tail_row = self.own_row + ZONE
        self.from_tail = j < before
        self.from_head = j >= AVG + after

    def take(self, ref, start, row, shift):
        a = ref[pl.ds(start + row, WIN), :]
        b = ref[pl.ds(start + row + 1, WIN), :]
        return pltpu.roll(
            jnp.where(self.lane >= shift, a, b), jnp.bitwise_and(LANES - shift, LANES - 1), 1
        )

    def __call__(self, own, own_at, tail, tail_at, head, head_at):
        mine = self.take(own, own_at, self.own_row, self.own_lane)
        prev = self.take(tail, tail_at, self.tail_row, self.own_lane)
        after = self.take(head, head_at, self.head_row, self.head_lane)
        return jnp.where(self.from_tail, prev, jnp.where(self.from_head, after, mine))


def drifts(held_ref, before_refs):
    before = before_refs[0][0, 0] - lax.axis_index("curve") * AVG
    return before, before + held_ref[0, 0] - AVG


def send_faces(low, high, even_out, odd_out, sem):
    even = is_even("grp")

    @pl.when(even)
    def _():
        run_copies([(high, even_out), (low, odd_out)], sem)

    @pl.when(jnp.logical_not(even))
    def _():
        run_copies([(low, even_out), (high, odd_out)], sem)


def take_faces(even_in, odd_in, low, high, sem):
    even = is_even("grp")

    @pl.when(even)
    def _():
        run_copies([(odd_in, low), (even_in, high)], sem)

    @pl.when(jnp.logical_not(even))
    def _():
        run_copies([(even_in, low), (odd_in, high)], sem)


def align_kernel(
    held_ref, before_refs, own, even_in, odd_in,
    even_out, odd_out, faces, sides,
    tail, head, edges, sem,
):
    before, after = drifts(held_ref, before_refs)
    even = is_even("curve")
    edge = 2 * 64 * ZONE
    zone = pl.ds(PAD, edge)
    take_zones(
        even_in.at[pl.ds(0, edge)], odd_in.at[pl.ds(0, edge)], tail.at[zone], head.at[zone], sem, even
    )
    packed = pl.ds(edge, 8)
    take_zones(even_in.at[packed], odd_in.at[packed], edges.at[0], edges.at[1], sem, even)
    here = Window(before, after)

    def body(k, carry):
        for z in range(8):
            i = k * 8 + z
            at = PAD + i * OWN
            zat = PAD + i * ZONE
            faces[pl.ds(pl.multiple_of(i * WIN, 8), WIN), :] = here(own, at, tail, zat, head, zat)
        return carry

    lax.fori_loop(0, 16, body, 0)
    lower = Window(before + 1, after + 1)
    upper = Window(before - 1, after - 1)
    j = here.row * LANES + here.lane
    for side, window, x, lost in (
        (0, lower, 7, jnp.logical_and(j == 0, before == HALF)),
        (1, upper, 0, jnp.logical_and(j == AVG - 1, after == -HALF)),
    ):
        beyond = spread(edges[side, 1:2, :])[64:]
        for plane in range(2):
            for z in range(8):
                i = (plane * 8 + x) * 8 + z
                at = PAD + i * OWN
                zat = PAD + i * ZONE
                value = window(own, at, tail, zat, head, zat)
                y = 56 * plane + z
                value = jnp.where(lost, beyond[y : y + 1], value)
                sides[pl.ds(((side * 2 + plane) * 8 + z) * WIN, WIN), :] = value
    half = 64 * WIN
    send_faces(faces.at[pl.ds(0, half)], faces.at[pl.ds(half, half)], even_out, odd_out, sem)


def each_x(run):
    run(0, 0)

    def mid(x, carry):
        run(x, 1)
        return carry

    lax.fori_loop(1, 7, mid, 0)
    run(7, 2)


def cell_rows(plane, x, z):
    at = ((plane * 8 + x) * 8 + z) * WIN
    return pl.ds(at if isinstance(at, int) else pl.multiple_of(at, 8), WIN)


def face_kernel(
    held_ref, before_refs, own, even_in, odd_in, even_face, odd_face, faces, sides,
    even_out, odd_out, even_end, odd_end, new, below, inner,
    tail, head, near, q, ends, sem,
):
    before, after = drifts(held_ref, before_refs)
    even = is_even("curve")
    size = 6 * 64 * ZONE
    half = 64 * WIN
    zone = pl.ds(PAD, size)
    take_zones(even_in, odd_in, tail.at[zone], head.at[zone], sem, even)
    take_faces(even_face, odd_face, near.at[pl.ds(0, half)], near.at[pl.ds(half, half)], sem)
    here = Window(before, after)

    def body(k, carry):
        for plane, ref, to, add in (
            (0, q, 0, 0.0),
            (5, q, 1, 0.0),
            (1, below, 0, 6.0),
            (4, below, 1, 6.0),
            (2, inner, 0, 6.0),
            (3, inner, 1, 6.0),
        ):
            for z in range(8):
                i = k * 8 + z
                at = PAD + ((plane + 2) * 64 + i) * OWN
                zat = PAD + (plane * 64 + i) * ZONE
                value = here(own, at, tail, zat, head, zat)
                ref[pl.ds(pl.multiple_of((to * 64 + i) * WIN, 8), WIN), :] = value + add
        return carry

    lax.fori_loop(0, 8, body, 0)

    def run(x, kind):
        for plane in range(2):
            for z in range(8):
                here = cell_rows(plane, x, z)
                total = q[here, :] + near[here, :]
                if kind == 0:
                    total += sides[pl.ds((plane * 8 + z) * WIN, WIN), :]
                else:
                    total += faces[cell_rows(plane, x - 1, z), :]
                if kind == 2:
                    total += sides[pl.ds(((2 + plane) * 8 + z) * WIN, WIN), :]
                else:
                    total += faces[cell_rows(plane, x + 1, z), :]
                if z > 0:
                    total += faces[cell_rows(plane, x, z - 1), :]
                if z < 7:
                    total += faces[cell_rows(plane, x, z + 1), :]
                new[here, :] = total / below[here, :]

    each_x(run)
    for plane in range(2):
        for z in range(8):
            i = plane * 8 + z
            ends[0, i : i + 1, :] = new[pl.ds(((plane * 8 + 7) * 8 + z) * WIN + WIN - 1, 1), :]
            ends[1, i : i + 1, :] = new[pl.ds((plane * 64 + z) * WIN, 1), :]
    send_faces(new.at[pl.ds(0, half)], new.at[pl.ds(half, half)], even_out, odd_out, sem)
    send_zones(ends.at[0], ends.at[1], even_end, odd_end, sem, even)


def last_kernel(
    held_ref, before_refs, own, even_in, odd_in, even_face, odd_face, even_end, odd_end,
    new, below, inner,
    out,
    tail, head, near, ends, sem,
):
    before, after = drifts(held_ref, before_refs)
    even = is_even("curve")
    size = 8 * 64 * ZONE
    half = 64 * WIN
    zone = pl.ds(PAD, size)
    take_zones(even_in, odd_in, tail.at[zone], head.at[zone], sem, even)
    take_zones(even_end, odd_end, ends.at[0], ends.at[1], sem, even)
    take_faces(even_face, odd_face, near.at[pl.ds(0, half)], near.at[pl.ds(half, half)], sem)
    here = Window(before, after)
    lane, row = here.lane, here.row

    def get(y, x, z):
        i = (y * 8 + x) * 8 + z
        return here(own, PAD + i * OWN, tail, PAD + i * ZONE, head, PAD + i * ZONE)

    def put(x, y, z, value):
        at = ((x * 8 + y) * 8 + z) * WIN
        out[pl.ds(at if isinstance(at, int) else pl.multiple_of(at, 8), WIN), :] = value

    def left(plane, z):
        v = pltpu.roll(new[cell_rows(plane, 7, z), :], 1, 1)
        i = plane * 8 + z
        edge = pltpu.roll(jnp.broadcast_to(ends[0, i : i + 1, :], (WIN, LANES)), 1, 1)
        return jnp.where(lane == 0, jnp.where(row == 0, edge, pltpu.roll(v, 1, 0)), v)

    def right(plane, z):
        v = pltpu.roll(new[cell_rows(plane, 0, z), :], LANES - 1, 1)
        i = plane * 8 + z
        edge = pltpu.roll(jnp.broadcast_to(ends[1, i : i + 1, :], (WIN, LANES)), LANES - 1, 1)
        next_row = jnp.where(row == WIN - 1, edge, pltpu.roll(v, WIN - 1, 0))
        return jnp.where(lane == LANES - 1, next_row, v)

    def run(x, kind):
        for plane, y in ((0, 0), (1, 7)):
            for z in range(8):
                cell = cell_rows(plane, x, z)
                total = get(y, x, z) + near[cell, :]
                total += left(plane, z) if kind == 0 else new[cell_rows(plane, x - 1, z), :]
                total += right(plane, z) if kind == 2 else new[cell_rows(plane, x + 1, z), :]
                if z > 0:
                    total += new[cell_rows(plane, x, z - 1), :]
                if z < 7:
                    total += new[cell_rows(plane, x, z + 1), :]
                put(x, y, z, total / below[cell, :])
        for plane, y in ((0, 1), (1, 6)):
            for z in range(8):
                cell = cell_rows(plane, x, z)
                put(x, y, z, (get(y, x, z) + new[cell, :]) / inner[cell, :])
        for y in range(2, 6):
            for z in range(8):
                put(x, y, z, get(y, x, z))

    each_x(run)


def swapped(value, axis, first):
    count = lax.axis_size(axis)
    pairs = [(i, i + 1) for i in range(first, count - 1, 2)]
    return lax.ppermute(value, axis, pairs + [(b, a) for a, b in pairs])


def swaps(values, axis):
    got = []
    for first, value in enumerate(values):
        got.append(swapped(value, axis, first))
    return got


def held_before(counts):
    rank, count = lax.axis_index("curve"), lax.axis_size("curve")
    places = [i for i in range(count) if 1 << i < count]
    above = [jnp.bitwise_and(rank >> i, 1).reshape(1, 1) for i in places]
    total, *above = lax.optimization_barrier((counts, *above))
    before = jnp.zeros_like(counts)
    for i in places:
        pairs = [(a, a ^ 1 << i) for a in range(count) if a ^ 1 << i < count]
        other = lax.ppermute(total, "curve", pairs)
        before += above[i] * other
        total += other
    return before


def array(*shape):
    return jax.ShapeDtypeStruct(shape, F32)


def call(kernel, outs, ins, scratch, limit, vmem_ins=(), vmem_outs=(), hbm_ins=(), us=2):
    (held,), others, *arrays = ins
    vmem = pl.BlockSpec(memory_space=pltpu.VMEM)
    specs = [SMEM] * (1 + len(others))
    specs += [
        vmem if i in vmem_ins else HBM if i in hbm_ins else ANY for i in range(len(arrays))
    ]

    def body(held_ref, *refs):
        kernel(held_ref, refs[: len(others)], *refs[len(others) :])

    return pl.pallas_call(
        body,
        out_shape=outs,
        in_specs=specs,
        out_specs=[vmem if i in vmem_outs else ANY for i in range(len(outs))],
        scratch_shapes=[pltpu.VMEM(shape, F32) for shape in scratch] + [pltpu.SemaphoreType.DMA((8,))],
        compiler_params=pltpu.CompilerParams(vmem_limit_bytes=limit * 2**20),
        cost_estimate=pl.CostEstimate(flops=us * 4_000_000, bytes_accessed=us * 10**6, transcendentals=0),
    )(held, *others, *arrays)


def local(state, coef, counts):
    state2 = state.reshape(2 * CELLS * OWN, LANES)
    coef2 = coef.reshape(CELLS * OWN, LANES)
    rows = CELLS * OWN
    zone = 64 * ZONE
    win = 64 * WIN

    others = (held_before(counts),)
    message, rest = (2 * zone + 8, LANES), (6 * zone, LANES)
    *faces_out, rest_a, rest_b = call(
        front_kernel,
        [array(*message)] * 2 + [array(*rest)] * 2,
        ((counts,), (), state2, coef2),
        [message, message, rest, rest],
        limit=4,
        vmem_ins=(0, 1),
    )
    faces_in = swaps(faces_out, "curve")
    rest_in = swaps((rest_a, rest_b), "curve")
    message = (8 * zone, LANES)
    front, pack, *sweep_out = call(
        sweep_kernel,
        [array(rows + 2 * PAD, LANES)] * 2 + [array(*message)] * 2,
        ((counts,), (), state2, coef2, *faces_in),
        [(rows + 2 * PAD, LANES), (2, 8, LANES), message, message],
        limit=24,
        vmem_ins=(0, 1),
        vmem_outs=(0, 1),
        us=6,
    )
    sweep_in = swaps(sweep_out, "curve")
    *near_out, faces, sides = call(
        align_kernel,
        [array(win, LANES)] * 2 + [array(2 * win, LANES), array(32 * WIN, LANES)],
        ((counts,), others, front, *faces_in),
        [(2 * zone + 2 * PAD, LANES), (2 * zone + 2 * PAD, LANES), (2, 8, LANES)],
        limit=8,
        vmem_ins=(0,),
        vmem_outs=(2, 3),
    )
    near_in = swaps(near_out, "grp")
    near_a, near_b, end_a, end_b, new, below, inner = call(
        face_kernel,
        [array(win, LANES)] * 2 + [array(16, LANES)] * 2 + [array(2 * win, LANES)] * 3,
        ((counts,), others, front, *rest_in, *near_in, faces, sides),
        [
            (6 * zone + 2 * PAD, LANES), (6 * zone + 2 * PAD, LANES),
            (2 * win, LANES), (2 * win, LANES), (2, 16, LANES),
        ],
        limit=8,
        vmem_ins=(0, 5, 6),
        vmem_outs=(4, 5, 6),
        us=3,
    )
    near_in = swaps((near_a, near_b), "grp")
    end_in = swaps((end_a, end_b), "curve")
    (out,) = call(
        last_kernel,
        [array(CELLS * WIN, LANES)],
        ((counts,), others, pack, *sweep_in, *near_in, *end_in, new, below, inner),
        [
            (8 * zone + 2 * PAD, LANES), (8 * zone + 2 * PAD, LANES),
            (2 * win, LANES), (2, 16, LANES),
        ],
        limit=12,
        vmem_ins=(0, 7, 8, 9),
        vmem_outs=(0,),
        us=3,
    )
    return out.reshape(CELLS, 1, AVG)


def solution(mesh):
    placed = (P(None, None, "grp", "curve"), P(None, "grp", "curve"), P("grp", "curve"))

    return jax.shard_map(
        local, mesh=mesh, in_specs=placed, out_specs=P(None, "grp", "curve"), check_vma=False
    )
```

```python
import jax
import jax.numpy as jnp
from jax import lax
from jax.experimental import pallas as pl
from jax.experimental.pallas import tpu as pltpu
from jax.sharding import PartitionSpec as P


AVG = 1024
HALF = 256
CAP = 1536

LANES = 128
OWN = CAP // LANES
ZONE = HALF // LANES
WIN = AVG // LANES
SLAB = 8 * OWN
CELLS = 512
PAD = 16
PLANE = 64 * ZONE
F32 = jnp.float32
ANY = pl.BlockSpec(memory_space=pl.ANY)
HBM = pl.BlockSpec(memory_space=pltpu.HBM)
SMEM = pl.BlockSpec(memory_space=pltpu.SMEM)


def iota(shape, dim):
    return lax.broadcasted_iota(jnp.int32, shape, dim)


def copies(pairs, sems):
    return [pltpu.make_async_copy(a, b, sems.at[i]) for i, (a, b) in enumerate(pairs)]


def run_copies(pairs, sems):
    todo = copies(pairs, sems)
    for copy in todo:
        copy.start()
    for copy in todo:
        copy.wait()


def tail_place(held):
    first = held - HALF
    return lax.div(first, LANES), lax.rem(first, LANES)


def put_zones(load, tail, head, base, place):
    row, shift = place
    lane = iota((8, LANES), 1)
    for i in range(ZONE):
        head[pl.ds(base + i, 8, stride=ZONE), :] = load(i)
    rows = [load(jnp.minimum(row + i, OWN - 1)) for i in range(ZONE + 1)]
    back = lax.rem(LANES - shift, LANES)
    for i in range(ZONE):
        both = jnp.where(lane >= shift, rows[i], rows[i + 1])
        tail[pl.ds(base + i, 8, stride=ZONE), :] = pltpu.roll(both, back, 1)


def send_zones(tail, head, even_out, odd_out, sem, even):
    @pl.when(even)
    def _():
        run_copies([(tail, even_out), (head, odd_out)], sem)

    @pl.when(jnp.logical_not(even))
    def _():
        run_copies([(head, even_out), (tail, odd_out)], sem)


def take_zones(even_in, odd_in, tail, head, sem, even):
    @pl.when(even)
    def _():
        run_copies([(odd_in, tail), (even_in, head)], sem)

    @pl.when(jnp.logical_not(even))
    def _():
        run_copies([(even_in, tail), (odd_in, head)], sem)


def is_even(axis):
    return lax.rem(lax.axis_index(axis), 2) == 0


def up8(v):
    n = v.shape[0]
    z = lax.rem(iota(v.shape, 0), 8)
    return jnp.where(z < 7, pltpu.roll(v, n - 1, 0), 0.0)


def down8(v):
    z = lax.rem(iota(v.shape, 0), 8)
    return jnp.where(z > 0, pltpu.roll(v, 1, 0), 0.0)


def edge_rows(u_ref, s_ref, c_ref, outer, row, lane, extra_row):
    inner = 6 if outer == 7 else 1

    def at(ref, x, r):
        return ref[pl.ds(x * 8 * SLAB + r, 64, stride=OWN), :]

    u = at(u_ref, outer, row)
    side = at(s_ref, outer, row) + at(u_ref, inner, row) + up8(u) + down8(u)
    zero = jnp.zeros((8, LANES), F32)
    side += jnp.concatenate([zero, u[:-8]], 0) + jnp.concatenate([u[8:], zero], 0)
    parts = [(u, side), (at(c_ref, outer, row), at(u_ref, outer, extra_row))]
    back = lax.rem(LANES - lane, LANES)
    rows = []
    for pair in parts:
        square = pltpu.roll(jnp.concatenate(pair, 0), back, 1)
        rows.append(jnp.transpose(square)[0:1])
    return rows


def spread(packed):
    return jnp.transpose(jnp.broadcast_to(packed, (LANES, LANES)))


def end_curves():
    curve = lax.axis_index("grp")
    return curve == 0, curve == lax.axis_size("grp") - 1


def plane_of(inner, low, high):
    first, last = end_curves()
    plane = jnp.where(first, high, jnp.where(last, low, inner))
    return pl.multiple_of(plane * PLANE, 8)


def front_kernel(
    held_ref, _, state, coef,
    even_1, odd_1, even_3, odd_3,
    tail, head, tail_edge, head_edge, sem,
):
    held = held_ref[0, 0]
    rows = CELLS * OWN
    u, c = state, coef
    s = state.at[pl.ds(rows, rows)]
    place = tail_place(held)
    even = is_even("curve")
    end = held - 1
    row, lane = lax.div(end, LANES), lax.rem(end, LANES)
    blank = jnp.zeros((6, LANES), F32)
    first = edge_rows(u, s, c, 0, 0, 0, ZONE)
    head_edge[...] = jnp.concatenate(first + [blank], 0)
    last = edge_rows(u, s, c, 7, row, lane, row - ZONE)
    tail_edge[...] = jnp.concatenate(last + [blank], 0)

    def at(ref, x, y):
        start = (x * 8 + y) * SLAB
        return lambda r: ref[pl.ds(start + r, 8, stride=OWN), :]

    def both(x, y, inner):
        return lambda r: at(u, x, inner)(r) + at(s, x, y)(r)

    for x in range(8):
        loads = [at(u, x, 0), at(u, x, 7), both(x, 0, 1), both(x, 7, 6)]
        loads += [at(c, x, y) for y in (0, 1, 7, 6)]
        for plane, load in enumerate(loads):
            put_zones(load, tail, head, (plane * 8 + x) * 8 * ZONE, place)

    def out(zone, edge, message_1, message_3):
        return [
            (zone.at[pl.ds(plane_of(0, 0, 1), PLANE)], message_1.at[pl.ds(0, PLANE)]),
            (zone.at[pl.ds(plane_of(1, 2, 3), PLANE)], message_1.at[pl.ds(PLANE, PLANE)]),
            (zone.at[pl.ds(plane_of(2, 4, 6), 2 * PLANE)], message_1.at[pl.ds(2 * PLANE, 2 * PLANE)]),
            (edge, message_1.at[pl.ds(4 * PLANE, 8)]),
            (zone.at[pl.ds(4 * PLANE, 4 * PLANE)], message_3),
        ]

    for flag, t, h in (
        (even, (even_1, even_3), (odd_1, odd_3)),
        (jnp.logical_not(even), (odd_1, odd_3), (even_1, even_3)),
    ):
        @pl.when(flag)
        def _():
            run_copies(out(tail, tail_edge, *t) + out(head, head_edge, *h), sem)


def take_edges(even_1, odd_1, edges, sem):
    rows = pl.ds(4 * PLANE, 8)
    take_zones(even_1.at[rows], odd_1.at[rows], edges.at[0], edges.at[1], sem, is_even("curve"))


def by_parity(evens, odds, tail, head, copies_in, sem):
    even = is_even("curve")
    for flag, t, h in ((even, odds, evens), (jnp.logical_not(even), evens, odds)):
        @pl.when(flag)
        def _():
            run_copies(copies_in(tail, *t) + copies_in(head, *h), sem)


def to_plane(zone, start, count=1):
    return zone.at[pl.ds(pl.multiple_of(PAD + start, 8), count * PLANE)]


def sweep_kernel(
    held_ref, _, state, coef,
    front, pack, ends,
    v, sem,
):
    held = held_ref[0, 0]
    first_curve, last_curve = end_curves()
    outer_sides = ((first_curve, 0, 1), (last_curve, 7, 6))
    u, c = state, coef
    s = state.at[pl.ds(CELLS * OWN, CELLS * OWN)]
    w = pack.at[pl.ds(PAD, CELLS * OWN)]
    row96 = iota((SLAB, LANES), 0)
    lane96 = iota((SLAB, LANES), 1)
    slot = lax.rem(row96, OWN) * LANES + lane96
    zlast, zfirst = row96 >= SLAB - OWN, row96 < OWN
    last_lane, first_lane = lane96 == LANES - 1, lane96 == 0
    starts = slot == 0
    finish = slot == held - 1

    def zsum(ref, b):
        up = jnp.where(zlast, 0.0, ref[pl.ds(b + OWN, SLAB), :])
        down = jnp.where(zfirst, 0.0, ref[pl.ds(b - OWN, SLAB), :])
        return up + down

    step = 8 * SLAB

    def left(ref, b):
        both = jnp.where(last_lane, ref[pl.ds(b - 1, SLAB), :], ref[pl.ds(b, SLAB), :])
        return jnp.where(starts, 0.0, pltpu.roll(both, 1, 1))

    def right(ref, b):
        both = jnp.where(first_lane, ref[pl.ds(b + 1, SLAB), :], ref[pl.ds(b, SLAB), :])
        return jnp.where(finish, 0.0, pltpu.roll(both, LANES - 1, 1))

    def xsum(ref, b, kind):
        if kind == 0:
            return left(ref, b + 7 * step) + ref[pl.ds(b + step, SLAB), :]
        if kind == 2:
            return ref[pl.ds(b - step, SLAB), :] + right(ref, b - 7 * step)
        return ref[pl.ds(b - step, SLAB), :] + ref[pl.ds(b + step, SLAB), :]

    def first(x, kind):
        def body(y, carry):
            b = (x * 8 + y) * SLAB
            if not isinstance(b, int):
                b = pl.multiple_of(b, 8)
            total = s[pl.ds(b, SLAB), :] + zsum(u, b) + xsum(u, b, kind)
            total += u[pl.ds(b - SLAB, SLAB), :] + u[pl.ds(b + SLAB, SLAB), :]
            v[pl.ds(b + PAD, SLAB), :] = total / (6.0 + c[pl.ds(b, SLAB), :])
            return carry

        lax.fori_loop(1, 7, body, 0)

    each_x(first)

    def slab(ref, x, y, off=0):
        b = off + (x * 8 + y) * SLAB
        return ref[pl.ds(b if isinstance(b, int) else pl.multiple_of(b, 8), SLAB), :]

    def zroll(value):
        up = jnp.where(zlast, 0.0, pltpu.roll(value, SLAB - OWN, 0))
        return up + jnp.where(zfirst, 0.0, pltpu.roll(value, OWN, 0))

    for outer, y, inner in outer_sides:
        @pl.when(outer)
        def _():
            def run(x, kind):
                b = (x * 8 + y) * SLAB
                b = b if isinstance(b, int) else pl.multiple_of(b, 8)
                total = slab(s, x, y) + zroll(slab(u, x, y)) + slab(u, x, inner) + xsum(u, b, kind)
                v[pl.ds(b + PAD, SLAB), :] = total / (6.0 + slab(c, x, y))

            each_x(run)

    def second(x, kind):
        def at(y):
            b = (x * 8 + y) * SLAB
            if not isinstance(b, int):
                b = pl.multiple_of(b, 8)
            return b, b + PAD

        def put(y, value):
            o = (y * 8 + x) * SLAB
            if not isinstance(o, int):
                o = pl.multiple_of(o, 8)
            w[pl.ds(o, SLAB), :] = value

        for y, inner in ((0, 1), (7, 6)):
            put(y, s[pl.ds(at(y)[0], SLAB), :] + v[pl.ds(at(inner)[1], SLAB), :])
        for y, inner in ((1, 2), (6, 5)):
            b, p = at(y)
            total = s[pl.ds(b, SLAB), :] + zsum(v, p) + xsum(v, p, kind)
            put(y, total + v[pl.ds(at(inner)[1], SLAB), :])

        def body(y, carry):
            b = (x * 8 + y) * SLAB
            b = b if isinstance(b, int) else pl.multiple_of(b, 8)
            p = b + PAD
            total = s[pl.ds(b, SLAB), :] + zsum(v, p) + xsum(v, p, kind)
            total += v[pl.ds(p - SLAB, SLAB), :] + v[pl.ds(p + SLAB, SLAB), :]
            o = pl.multiple_of((y * 8 + x) * SLAB, 8)
            w[pl.ds(o, SLAB), :] = total / (6.0 + c[pl.ds(b, SLAB), :])
            return carry

        lax.fori_loop(2, 6, body, 0)

    each_x(second)

    for outer, y, inner in outer_sides:
        @pl.when(outer)
        def _():
            def run(x, kind):
                b = (x * 8 + y) * SLAB
                b = b if isinstance(b, int) else pl.multiple_of(b, 8)
                o = pl.ds((y * 8 + x) * SLAB, SLAB)
                total = slab(s, x, y) + zroll(slab(v, x, y, PAD)) + xsum(v, b + PAD, kind)
                total += slab(v, x, inner, PAD)
                w[o, :] = total / (6.0 + slab(c, x, y))
                o = pl.ds((inner * 8 + x) * SLAB, SLAB)
                w[o, :] = (w[o, :] + slab(v, x, y, PAD)) / (6.0 + slab(c, x, inner))

            each_x(run)

    end_row = lax.div(held - 1, LANES)
    for side, x, inner, at_row in ((0, 0, 1, 0), (1, 7, 6, end_row)):
        for i, (ref, at_x) in enumerate(((c, x), (c, inner), (u, x))):
            rows = pl.ds(at_x * step + at_row, 64, stride=OWN)
            ends[pl.ds((side * 3 + i) * 64, 64), :] = ref[rows, :]

    def keep(x, carry):
        def slab(ref, y):
            return ref[pl.ds(pl.multiple_of((x * 8 + y) * SLAB, 8), SLAB), :]

        for plane, value in enumerate(
            (
                slab(u, 0), slab(u, 7), slab(s, 0) + slab(u, 1), slab(s, 7) + slab(u, 6),
                slab(c, 0), slab(c, 1), slab(c, 7), slab(c, 6),
            )
        ):
            front[pl.ds(pl.multiple_of(PAD + (plane * 8 + x) * SLAB, 8), SLAB), :] = value
        return carry

    lax.fori_loop(0, 8, keep, 0)


def edge_kernel(
    held_ref, _, pack, ends, even_1, odd_1,
    new_pack, even_out, odd_out,
    edges, tail, head, sem,
):
    held = held_ref[0, 0]
    rank, ranks = lax.axis_index("curve"), lax.axis_size("curve")
    first_curve, last_curve = end_curves()
    take_edges(even_1, odd_1, edges, sem)
    w = new_pack.at[pl.ds(PAD, CELLS * OWN)]
    lane, row = iota((64, LANES), 1), iota((64, LANES), 0)
    lone = jnp.logical_or(
        jnp.logical_and(row < 8, jnp.logical_not(first_curve)),
        jnp.logical_and(row >= 56, jnp.logical_not(last_curve)),
    )
    plain = jnp.logical_or(
        jnp.logical_and(row < 16, jnp.logical_not(first_curve)),
        jnp.logical_and(row >= 48, jnp.logical_not(last_curve)),
    )
    end_row, end_lane = lax.div(held - 1, LANES), lax.rem(held - 1, LANES)
    zero = jnp.zeros((8, LANES), F32)
    for side, x, inner, at_row, at_lane, there in (
        (0, 0, 1, 0, 0, rank > 0),
        (1, 7, 6, end_row, end_lane, rank < ranks - 1),
    ):
        a = spread(edges[side, 0:1, :])
        b = spread(edges[side, 1:2, :])
        coef, coef_inner, field = [ends[pl.ds((side * 3 + i) * 64, 64), :] for i in range(3)]
        hit = jnp.logical_and(lane == at_lane, jnp.logical_not(lone))
        more = jnp.where(hit, a[:64] / (6.0 + coef), 0.0)
        beyond = (a[64:] + field) / (6.0 + b[:64])
        total = jnp.where(jnp.logical_and(hit, there), beyond, 0.0) + up8(more) + down8(more)
        total += jnp.concatenate([zero, more[:-8]], 0) + jnp.concatenate([more[8:], zero], 0)
        total = total / jnp.where(plain, 1.0, 6.0 + coef)
        more = more / jnp.where(plain, 1.0, 6.0 + coef_inner)
        for at_x, value in ((x, total), (inner, more)):
            for y in range(8):
                o = pl.ds((y * 8 + at_x) * SLAB + at_row, 8, stride=OWN)
                w[o, :] = w[o, :] + value[8 * y : 8 * y + 8]

    place = tail_place(held)

    def body(i, carry):
        for k in range(8):
            at = pl.multiple_of((i * 8 + k) * SLAB, 8)
            load = lambda r, at=at: w[pl.ds(at + r, 8, stride=OWN), :]
            put_zones(load, tail, head, pl.multiple_of((i * 8 + k) * 8 * ZONE, 8), place)
        return carry

    lax.fori_loop(0, 8, body, 0)
    send_zones(tail, head, even_out, odd_out, sem, is_even("curve"))


class Window:
    def __init__(self, before, after):
        self.lane = iota((WIN, LANES), 1)
        self.row = iota((WIN, LANES), 0)
        j = self.row * LANES + self.lane
        down = lambda n: lax.shift_right_arithmetic(n, 7)
        self.own_row = down(-before)
        self.own_lane = jnp.bitwise_and(-before, LANES - 1)
        self.head_row = down(-AVG - after)
        self.head_lane = jnp.bitwise_and(-AVG - after, LANES - 1)
        self.tail_row = self.own_row + ZONE
        self.from_tail = j < before
        self.from_head = j >= AVG + after

    def take(self, ref, start, row, shift):
        a = ref[pl.ds(start + row, WIN), :]
        b = ref[pl.ds(start + row + 1, WIN), :]
        return pltpu.roll(
            jnp.where(self.lane >= shift, a, b), jnp.bitwise_and(LANES - shift, LANES - 1), 1
        )

    def __call__(self, own, own_at, tail, tail_at, head, head_at):
        mine = self.take(own, own_at, self.own_row, self.own_lane)
        prev = self.take(tail, tail_at, self.tail_row, self.own_lane)
        after = self.take(head, head_at, self.head_row, self.head_lane)
        return jnp.where(self.from_tail, prev, jnp.where(self.from_head, after, mine))


def drifts(held_ref, before_refs):
    before = before_refs[0][0, 0] - lax.axis_index("curve") * AVG
    return before, before + held_ref[0, 0] - AVG


def send_faces(low, high, even_out, odd_out, sem):
    even = is_even("grp")

    @pl.when(even)
    def _():
        run_copies([(high, even_out), (low, odd_out)], sem)

    @pl.when(jnp.logical_not(even))
    def _():
        run_copies([(low, even_out), (high, odd_out)], sem)


def take_faces(even_in, odd_in, low, high, sem):
    even = is_even("grp")

    @pl.when(even)
    def _():
        run_copies([(odd_in, low), (even_in, high)], sem)

    @pl.when(jnp.logical_not(even))
    def _():
        run_copies([(even_in, low), (odd_in, high)], sem)


def align_kernel(
    held_ref, before_refs, own, even_1, odd_1,
    even_out, odd_out, faces, sides,
    tail, head, edges, sem,
):
    before, after = drifts(held_ref, before_refs)
    even = is_even("curve")

    def copies_in(zone, message):
        first, last = end_curves()
        other = pl.multiple_of(jnp.where(jnp.logical_or(first, last), 2 * PLANE, PLANE), 8)
        return [
            (message.at[pl.ds(0, PLANE)], to_plane(zone, plane_of(0, 0, 1))),
            (message.at[pl.ds(PLANE, PLANE)], to_plane(zone, other)),
        ]

    by_parity((even_1,), (odd_1,), tail, head, copies_in, sem)
    take_edges(even_1, odd_1, edges, sem)
    here = Window(before, after)

    def body(k, carry):
        for z in range(8):
            i = k * 8 + z
            at = PAD + i * OWN
            zat = PAD + i * ZONE
            faces[pl.ds(pl.multiple_of(i * WIN, 8), WIN), :] = here(own, at, tail, zat, head, zat)
        return carry

    lax.fori_loop(0, 16, body, 0)
    lower = Window(before + 1, after + 1)
    upper = Window(before - 1, after - 1)
    j = here.row * LANES + here.lane
    for side, window, x, lost in (
        (0, lower, 7, jnp.logical_and(j == 0, before == HALF)),
        (1, upper, 0, jnp.logical_and(j == AVG - 1, after == -HALF)),
    ):
        beyond = spread(edges[side, 1:2, :])[64:]
        for plane in range(2):
            for z in range(8):
                i = (plane * 8 + x) * 8 + z
                at = PAD + i * OWN
                zat = PAD + i * ZONE
                value = window(own, at, tail, zat, head, zat)
                y = 56 * plane + z
                value = jnp.where(lost, beyond[y : y + 1], value)
                sides[pl.ds(((side * 2 + plane) * 8 + z) * WIN, WIN), :] = value
    half = 64 * WIN
    send_faces(faces.at[pl.ds(0, half)], faces.at[pl.ds(half, half)], even_out, odd_out, sem)


def each_x(run):
    run(0, 0)

    def mid(x, carry):
        run(x, 1)
        return carry

    lax.fori_loop(1, 7, mid, 0)
    run(7, 2)


def cell_rows(plane, x, z):
    at = ((plane * 8 + x) * 8 + z) * WIN
    return pl.ds(at if isinstance(at, int) else pl.multiple_of(at, 8), WIN)


def face_kernel(
    held_ref, before_refs, own, even_1, odd_1, even_3, odd_3,
    even_face, odd_face, faces, sides,
    even_out, odd_out, even_end, odd_end, new, below, inner,
    tail, head, near, q, ends, sem,
):
    before, after = drifts(held_ref, before_refs)
    even = is_even("curve")
    half = 64 * WIN

    def copies_in(zone, message_1, message_3):
        first, last = end_curves()
        rest = jnp.where(jnp.logical_or(first, last), 8 * PLANE, 4 * PLANE)
        return [
            (message_1.at[pl.ds(PLANE, PLANE)], to_plane(zone, plane_of(1, 2, 3))),
            (message_1.at[pl.ds(2 * PLANE, 2 * PLANE)], to_plane(zone, plane_of(2, 4, 6), 2)),
            (message_3, to_plane(zone, rest, 4)),
        ]

    by_parity((even_1, even_3), (odd_1, odd_3), tail, head, copies_in, sem)
    take_faces(even_face, odd_face, near.at[pl.ds(0, half)], near.at[pl.ds(half, half)], sem)
    here = Window(before, after)

    def body(k, carry):
        for plane, ref, to, add in (
            (2, q, 0, 0.0),
            (3, q, 1, 0.0),
            (4, below, 0, 6.0),
            (6, below, 1, 6.0),
            (5, inner, 0, 6.0),
            (7, inner, 1, 6.0),
        ):
            for z in range(8):
                i = k * 8 + z
                at = PAD + (plane * 64 + i) * OWN
                zat = PAD + (plane * 64 + i) * ZONE
                value = here(own, at, tail, zat, head, zat)
                ref[pl.ds(pl.multiple_of((to * 64 + i) * WIN, 8), WIN), :] = value + add
        return carry

    lax.fori_loop(0, 8, body, 0)

    def run(x, kind):
        for plane in range(2):
            for z in range(8):
                here = cell_rows(plane, x, z)
                total = q[here, :] + near[here, :]
                if kind == 0:
                    total += sides[pl.ds((plane * 8 + z) * WIN, WIN), :]
                else:
                    total += faces[cell_rows(plane, x - 1, z), :]
                if kind == 2:
                    total += sides[pl.ds(((2 + plane) * 8 + z) * WIN, WIN), :]
                else:
                    total += faces[cell_rows(plane, x + 1, z), :]
                if z > 0:
                    total += faces[cell_rows(plane, x, z - 1), :]
                if z < 7:
                    total += faces[cell_rows(plane, x, z + 1), :]
                new[here, :] = total / below[here, :]

    each_x(run)
    for plane in range(2):
        for z in range(8):
            i = plane * 8 + z
            ends[0, i : i + 1, :] = new[pl.ds(((plane * 8 + 7) * 8 + z) * WIN + WIN - 1, 1), :]
            ends[1, i : i + 1, :] = new[pl.ds((plane * 64 + z) * WIN, 1), :]
    send_faces(new.at[pl.ds(0, half)], new.at[pl.ds(half, half)], even_out, odd_out, sem)
    send_zones(ends.at[0], ends.at[1], even_end, odd_end, sem, even)


def last_kernel(
    held_ref, before_refs, own, even_in, odd_in, even_face, odd_face, even_end, odd_end,
    new, below, inner,
    out,
    tail, head, near, ends, sem,
):
    before, after = drifts(held_ref, before_refs)
    even = is_even("curve")
    size = 8 * 64 * ZONE
    half = 64 * WIN
    zone = pl.ds(PAD, size)
    take_zones(even_in, odd_in, tail.at[zone], head.at[zone], sem, even)
    take_zones(even_end, odd_end, ends.at[0], ends.at[1], sem, even)
    take_faces(even_face, odd_face, near.at[pl.ds(0, half)], near.at[pl.ds(half, half)], sem)
    here = Window(before, after)
    lane, row = here.lane, here.row
    outer = end_curves()

    def get(y, x, z):
        i = (y * 8 + x) * 8 + z
        return here(own, PAD + i * OWN, tail, PAD + i * ZONE, head, PAD + i * ZONE)

    def put(x, y, z, value):
        at = ((x * 8 + y) * 8 + z) * WIN
        out[pl.ds(at if isinstance(at, int) else pl.multiple_of(at, 8), WIN), :] = value

    def left(plane, z):
        v = pltpu.roll(new[cell_rows(plane, 7, z), :], 1, 1)
        i = plane * 8 + z
        edge = pltpu.roll(jnp.broadcast_to(ends[0, i : i + 1, :], (WIN, LANES)), 1, 1)
        return jnp.where(lane == 0, jnp.where(row == 0, edge, pltpu.roll(v, 1, 0)), v)

    def right(plane, z):
        v = pltpu.roll(new[cell_rows(plane, 0, z), :], LANES - 1, 1)
        i = plane * 8 + z
        edge = pltpu.roll(jnp.broadcast_to(ends[1, i : i + 1, :], (WIN, LANES)), LANES - 1, 1)
        next_row = jnp.where(row == WIN - 1, edge, pltpu.roll(v, WIN - 1, 0))
        return jnp.where(lane == LANES - 1, next_row, v)

    def run(x, kind):
        for plane, y in ((0, 0), (1, 7)):
            for z in range(8):
                cell = cell_rows(plane, x, z)
                held = get(y, x, z)
                total = held + near[cell, :]
                total += left(plane, z) if kind == 0 else new[cell_rows(plane, x - 1, z), :]
                total += right(plane, z) if kind == 2 else new[cell_rows(plane, x + 1, z), :]
                if z > 0:
                    total += new[cell_rows(plane, x, z - 1), :]
                if z < 7:
                    total += new[cell_rows(plane, x, z + 1), :]
                put(x, y, z, jnp.where(outer[plane], held, total / below[cell, :]))
        for plane, y in ((0, 1), (1, 6)):
            for z in range(8):
                cell = cell_rows(plane, x, z)
                held = get(y, x, z)
                total = (held + new[cell, :]) / inner[cell, :]
                put(x, y, z, jnp.where(outer[plane], held, total))
        for y in range(2, 6):
            for z in range(8):
                put(x, y, z, get(y, x, z))

    each_x(run)


def swapped(value, axis, first, inner):
    count = lax.axis_size(axis)
    pairs = [(i, i + 1) for i in range(first, count - 1, 2)]
    pairs += [(b, a) for a, b in pairs]
    if inner:
        curves = lax.axis_size("grp")
        pairs = [(a * curves + g, b * curves + g) for a, b in pairs for g in range(1, curves - 1)]
        axis = (axis, "grp")
    return lax.ppermute(value, axis, pairs)


def swaps(values, axis, inner=False):
    got = []
    for first, value in enumerate(values):
        got.append(swapped(value, axis, first, inner))
    return got


def held_before(counts):
    rank, count = lax.axis_index("curve"), lax.axis_size("curve")
    places = [i for i in range(count) if 1 << i < count]
    above = [jnp.bitwise_and(rank >> i, 1).reshape(1, 1) for i in places]
    total, *above = lax.optimization_barrier((counts, *above))
    before = jnp.zeros_like(counts)
    for i in places[:-1]:
        pairs = [(a, a ^ 1 << i) for a in range(count) if a ^ 1 << i < count]
        other = lax.ppermute(total, "curve", pairs)
        before += above[i] * other
        total += other
    for top in above[len(places) - 1 :]:
        before += top * (count * AVG - total)
    return before


def array(*shape):
    return jax.ShapeDtypeStruct(shape, F32)


def call(kernel, outs, ins, scratch, limit, vmem_ins=(), vmem_outs=(), hbm_ins=(), us=2, aliases={}):
    (held,), others, *arrays = ins
    vmem = pl.BlockSpec(memory_space=pltpu.VMEM)
    specs = [SMEM] * (1 + len(others))
    specs += [
        vmem if i in vmem_ins else HBM if i in hbm_ins else ANY for i in range(len(arrays))
    ]

    def body(held_ref, *refs):
        kernel(held_ref, refs[: len(others)], *refs[len(others) :])

    return pl.pallas_call(
        body,
        out_shape=outs,
        in_specs=specs,
        out_specs=[vmem if i in vmem_outs else ANY for i in range(len(outs))],
        scratch_shapes=[pltpu.VMEM(shape, F32) for shape in scratch] + [pltpu.SemaphoreType.DMA((10,))],
        compiler_params=pltpu.CompilerParams(vmem_limit_bytes=limit * 2**20),
        cost_estimate=pl.CostEstimate(flops=us * 4_000_000, bytes_accessed=us * 10**6, transcendentals=0),
        input_output_aliases=aliases,
    )(held, *others, *arrays)


def local(state, coef, counts):
    state2 = state.reshape(2 * CELLS * OWN, LANES)
    coef2 = coef.reshape(CELLS * OWN, LANES)
    rows = CELLS * OWN
    zone = 64 * ZONE
    win = 64 * WIN

    others = (held_before(counts),)
    message, edge = (8 * zone, LANES), (8, LANES)
    outs = call(
        front_kernel,
        [array(4 * zone + 8, LANES)] * 2 + [array(4 * zone, LANES)] * 2,
        ((counts,), (), state2, coef2),
        [message, message, edge, edge],
        limit=6,
        vmem_ins=(0, 1),
    )
    in_1 = swaps(outs[:2], "curve")
    in_3 = swaps(outs[2:], "curve", inner=True)
    front, pack, ends = call(
        sweep_kernel,
        [array(rows + 2 * PAD, LANES)] * 2 + [array(6 * 64, LANES)],
        ((counts,), (), state2, coef2),
        [(rows + 2 * PAD, LANES)],
        limit=16,
        vmem_ins=(0, 1),
        vmem_outs=(0, 1, 2),
        us=6,
    )
    pack, *sweep_out = call(
        edge_kernel,
        [array(rows + 2 * PAD, LANES)] + [array(*message)] * 2,
        ((counts,), (), pack, ends, *in_1),
        [(2, 8, LANES), message, message],
        limit=8,
        vmem_ins=(0, 1),
        vmem_outs=(0,),
        aliases={1: 0},
    )
    sweep_in = swaps(sweep_out, "curve")
    *near_out, faces, sides = call(
        align_kernel,
        [array(win, LANES)] * 2 + [array(2 * win, LANES), array(32 * WIN, LANES)],
        ((counts,), others, front, *in_1),
        [(3 * zone + 2 * PAD, LANES), (3 * zone + 2 * PAD, LANES), (2, 8, LANES)],
        limit=8,
        vmem_ins=(0,),
        vmem_outs=(2, 3),
    )
    near_in = swaps(near_out, "grp")
    near_a, near_b, end_a, end_b, new, below, inner = call(
        face_kernel,
        [array(win, LANES)] * 2 + [array(16, LANES)] * 2 + [array(2 * win, LANES)] * 3,
        ((counts,), others, front, *in_1, *in_3, *near_in, faces, sides),
        [
            (12 * zone + 2 * PAD, LANES), (12 * zone + 2 * PAD, LANES),
            (2 * win, LANES), (2 * win, LANES), (2, 16, LANES),
        ],
        limit=8,
        vmem_ins=(0, 7, 8),
        vmem_outs=(4, 5, 6),
        us=3,
    )
    near_in = swaps((near_a, near_b), "grp")
    end_in = swaps((end_a, end_b), "curve")
    (out,) = call(
        last_kernel,
        [array(CELLS * WIN, LANES)],
        ((counts,), others, pack, *sweep_in, *near_in, *end_in, new, below, inner),
        [
            (8 * zone + 2 * PAD, LANES), (8 * zone + 2 * PAD, LANES),
            (2 * win, LANES), (2, 16, LANES),
        ],
        limit=12,
        vmem_ins=(0, 7, 8, 9),
        vmem_outs=(0,),
        us=3,
    )
    return out.reshape(CELLS, 1, AVG)


def solution(mesh):
    placed = (P(None, None, "grp", "curve"), P(None, "grp", "curve"), P("grp", "curve"))

    return jax.shard_map(
        local, mesh=mesh, in_specs=placed, out_specs=P(None, "grp", "curve"), check_vma=False
    )
```

```python
import jax
import jax.numpy as jnp
from jax import lax
from jax.experimental import pallas as pl
from jax.experimental.pallas import tpu as pltpu
from jax.sharding import PartitionSpec as P


AVG = 1024
HALF = 256
CAP = 1536

LANES = 128
OWN = CAP // LANES
ZONE = HALF // LANES
WIN = AVG // LANES
SLAB = 8 * OWN
CELLS = 512
PAD = 16
PLANE = 64 * ZONE
F32 = jnp.float32
ANY = pl.BlockSpec(memory_space=pl.ANY)
HBM = pl.BlockSpec(memory_space=pltpu.HBM)
SMEM = pl.BlockSpec(memory_space=pltpu.SMEM)


def iota(shape, dim):
    return lax.broadcasted_iota(jnp.int32, shape, dim)


def copies(pairs, sems):
    return [pltpu.make_async_copy(a, b, sems.at[i]) for i, (a, b) in enumerate(pairs)]


def run_copies(pairs, sems):
    todo = copies(pairs, sems)
    for copy in todo:
        copy.start()
    for copy in todo:
        copy.wait()


def tail_place(held):
    first = held - HALF
    return lax.div(first, LANES), lax.rem(first, LANES)


def put_zones(load, tail, head, base, place):
    row, shift = place
    lane = iota((8, LANES), 1)
    for i in range(ZONE):
        head[pl.ds(base + i, 8, stride=ZONE), :] = load(i)
    rows = [load(jnp.minimum(row + i, OWN - 1)) for i in range(ZONE + 1)]
    back = lax.rem(LANES - shift, LANES)
    for i in range(ZONE):
        both = jnp.where(lane >= shift, rows[i], rows[i + 1])
        tail[pl.ds(base + i, 8, stride=ZONE), :] = pltpu.roll(both, back, 1)


def send_zones(tail, head, even_out, odd_out, sem, even):
    @pl.when(even)
    def _():
        run_copies([(tail, even_out), (head, odd_out)], sem)

    @pl.when(jnp.logical_not(even))
    def _():
        run_copies([(head, even_out), (tail, odd_out)], sem)


def take_zones(even_in, odd_in, tail, head, sem, even):
    @pl.when(even)
    def _():
        run_copies([(odd_in, tail), (even_in, head)], sem)

    @pl.when(jnp.logical_not(even))
    def _():
        run_copies([(even_in, tail), (odd_in, head)], sem)


def is_even(axis):
    return lax.rem(lax.axis_index(axis), 2) == 0


def up8(v):
    n = v.shape[0]
    z = lax.rem(iota(v.shape, 0), 8)
    return jnp.where(z < 7, pltpu.roll(v, n - 1, 0), 0.0)


def down8(v):
    z = lax.rem(iota(v.shape, 0), 8)
    return jnp.where(z > 0, pltpu.roll(v, 1, 0), 0.0)


def edge_rows(u_ref, s_ref, c_ref, outer, row, lane, extra_row):
    inner = 6 if outer == 7 else 1

    def at(ref, x, r):
        return ref[pl.ds(x * 8 * SLAB + r, 64, stride=OWN), :]

    u = at(u_ref, outer, row)
    side = at(s_ref, outer, row) + at(u_ref, inner, row) + up8(u) + down8(u)
    zero = jnp.zeros((8, LANES), F32)
    side += jnp.concatenate([zero, u[:-8]], 0) + jnp.concatenate([u[8:], zero], 0)
    parts = [(u, side), (at(c_ref, outer, row), at(u_ref, outer, extra_row))]
    back = lax.rem(LANES - lane, LANES)
    rows = []
    for pair in parts:
        square = pltpu.roll(jnp.concatenate(pair, 0), back, 1)
        rows.append(jnp.transpose(square)[0:1])
    return rows


def spread(packed):
    return jnp.transpose(jnp.broadcast_to(packed, (LANES, LANES)))


def end_curves():
    curve = lax.axis_index("grp")
    return curve == 0, curve == lax.axis_size("grp") - 1


def plane_of(inner, low, high):
    first, last = end_curves()
    plane = jnp.where(first, high, jnp.where(last, low, inner))
    return pl.multiple_of(plane * PLANE, 8)


def front_kernel(
    held_ref, _, state, coef,
    even_edge, odd_edge, even_1, odd_1, even_2, odd_2, count,
    tail, head, tail_edge, head_edge, sem,
):
    held = held_ref[0, 0]
    rows = CELLS * OWN
    u, c = state, coef
    s = state.at[pl.ds(rows, rows)]
    place = tail_place(held)
    even = is_even("curve")
    end = held - 1
    row, lane = lax.div(end, LANES), lax.rem(end, LANES)
    blank = jnp.zeros((6, LANES), F32)
    first = edge_rows(u, s, c, 0, 0, 0, ZONE)
    head_edge[...] = jnp.concatenate(first + [blank], 0)
    last = edge_rows(u, s, c, 7, row, lane, row - ZONE)
    tail_edge[...] = jnp.concatenate(last + [blank], 0)

    def at(ref, x, y):
        start = (x * 8 + y) * SLAB
        return lambda r: ref[pl.ds(start + r, 8, stride=OWN), :]

    def both(x, y, inner):
        return lambda r: at(u, x, inner)(r) + at(s, x, y)(r)

    for x in range(8):
        loads = [at(u, x, 0), at(u, x, 7), both(x, 0, 1), both(x, 7, 6)]
        loads += [at(c, x, y) for y in (0, 1, 7, 6)]
        for plane, load in enumerate(loads):
            put_zones(load, tail, head, (plane * 8 + x) * 8 * ZONE, place)

    count[...] = jnp.full((8, LANES), held, jnp.int32).astype(F32)

    def one_side(zone, message, _):
        return [
            (zone.at[pl.ds(plane_of(0, 0, 1), PLANE)], message.at[pl.ds(0, PLANE)]),
            (zone.at[pl.ds(plane_of(1, 2, 3), PLANE)], message.at[pl.ds(PLANE, PLANE)]),
            (zone.at[pl.ds(plane_of(2, 4, 6), 2 * PLANE)], message.at[pl.ds(2 * PLANE, 2 * PLANE)]),
        ]

    def both_sides(zone, _, message):
        return [(zone, message)]

    for flag, t, h, te, he in (
        (even, (even_1, even_2), (odd_1, odd_2), even_edge, odd_edge),
        (jnp.logical_not(even), (odd_1, odd_2), (even_1, even_2), odd_edge, even_edge),
    ):
        for kind, out in by_kind(one_side, both_sides):
            @pl.when(jnp.logical_and(flag, kind))
            def _():
                edges = [(tail_edge, te), (head_edge, he)]
                run_copies(edges + out(tail, *t) + out(head, *h), sem)


def by_kind(one_side, both_sides):
    first, last = end_curves()
    edge = jnp.logical_or(first, last)
    return (edge, one_side), (jnp.logical_not(edge), both_sides)


def by_parity(evens, odds, tail, head, one_side, both_sides, sem):
    even = is_even("curve")
    for flag, t, h in ((even, odds, evens), (jnp.logical_not(even), evens, odds)):
        for kind, to in by_kind(one_side, both_sides):
            @pl.when(jnp.logical_and(flag, kind))
            def _():
                run_copies(to(tail, *t) + to(head, *h), sem)


def to_plane(zone, start, count=1):
    return zone.at[pl.ds(pl.multiple_of(PAD + start, 8), count * PLANE)]


def sweep_kernel(
    held_ref, _, state, coef,
    front, pack, ends,
    v, sem,
):
    held = held_ref[0, 0]
    first_curve, last_curve = end_curves()
    outer_sides = ((first_curve, 0, 1), (last_curve, 7, 6))
    u, c = state, coef
    s = state.at[pl.ds(CELLS * OWN, CELLS * OWN)]
    w = pack.at[pl.ds(PAD, CELLS * OWN)]
    row96 = iota((SLAB, LANES), 0)
    lane96 = iota((SLAB, LANES), 1)
    slot = lax.rem(row96, OWN) * LANES + lane96
    zlast, zfirst = row96 >= SLAB - OWN, row96 < OWN
    last_lane, first_lane = lane96 == LANES - 1, lane96 == 0
    starts = slot == 0
    finish = slot == held - 1

    def zsum(ref, b):
        up = jnp.where(zlast, 0.0, ref[pl.ds(b + OWN, SLAB), :])
        down = jnp.where(zfirst, 0.0, ref[pl.ds(b - OWN, SLAB), :])
        return up + down

    step = 8 * SLAB

    def left(ref, b):
        both = jnp.where(last_lane, ref[pl.ds(b - 1, SLAB), :], ref[pl.ds(b, SLAB), :])
        return jnp.where(starts, 0.0, pltpu.roll(both, 1, 1))

    def right(ref, b):
        both = jnp.where(first_lane, ref[pl.ds(b + 1, SLAB), :], ref[pl.ds(b, SLAB), :])
        return jnp.where(finish, 0.0, pltpu.roll(both, LANES - 1, 1))

    def xsum(ref, b, kind):
        if kind == 0:
            return left(ref, b + 7 * step) + ref[pl.ds(b + step, SLAB), :]
        if kind == 2:
            return ref[pl.ds(b - step, SLAB), :] + right(ref, b - 7 * step)
        return ref[pl.ds(b - step, SLAB), :] + ref[pl.ds(b + step, SLAB), :]

    def first(x, kind):
        def body(y, carry):
            b = (x * 8 + y) * SLAB
            if not isinstance(b, int):
                b = pl.multiple_of(b, 8)
            total = s[pl.ds(b, SLAB), :] + zsum(u, b) + xsum(u, b, kind)
            total += u[pl.ds(b - SLAB, SLAB), :] + u[pl.ds(b + SLAB, SLAB), :]
            v[pl.ds(b + PAD, SLAB), :] = total / (6.0 + c[pl.ds(b, SLAB), :])
            return carry

        lax.fori_loop(1, 7, body, 0)

    each_x(first)

    def slab(ref, x, y, off=0):
        b = off + (x * 8 + y) * SLAB
        return ref[pl.ds(b if isinstance(b, int) else pl.multiple_of(b, 8), SLAB), :]

    def zroll(value):
        up = jnp.where(zlast, 0.0, pltpu.roll(value, SLAB - OWN, 0))
        return up + jnp.where(zfirst, 0.0, pltpu.roll(value, OWN, 0))

    for outer, y, inner in outer_sides:
        @pl.when(outer)
        def _():
            def run(x, kind):
                b = (x * 8 + y) * SLAB
                b = b if isinstance(b, int) else pl.multiple_of(b, 8)
                total = slab(s, x, y) + zroll(slab(u, x, y)) + slab(u, x, inner) + xsum(u, b, kind)
                v[pl.ds(b + PAD, SLAB), :] = total / (6.0 + slab(c, x, y))

            each_x(run)

    def second(x, kind):
        def at(y):
            b = (x * 8 + y) * SLAB
            if not isinstance(b, int):
                b = pl.multiple_of(b, 8)
            return b, b + PAD

        def put(y, value):
            o = (y * 8 + x) * SLAB
            if not isinstance(o, int):
                o = pl.multiple_of(o, 8)
            w[pl.ds(o, SLAB), :] = value

        for y, inner in ((0, 1), (7, 6)):
            put(y, s[pl.ds(at(y)[0], SLAB), :] + v[pl.ds(at(inner)[1], SLAB), :])
        for y, inner in ((1, 2), (6, 5)):
            b, p = at(y)
            total = s[pl.ds(b, SLAB), :] + zsum(v, p) + xsum(v, p, kind)
            put(y, total + v[pl.ds(at(inner)[1], SLAB), :])

        def body(y, carry):
            b = (x * 8 + y) * SLAB
            b = b if isinstance(b, int) else pl.multiple_of(b, 8)
            p = b + PAD
            total = s[pl.ds(b, SLAB), :] + zsum(v, p) + xsum(v, p, kind)
            total += v[pl.ds(p - SLAB, SLAB), :] + v[pl.ds(p + SLAB, SLAB), :]
            o = pl.multiple_of((y * 8 + x) * SLAB, 8)
            w[pl.ds(o, SLAB), :] = total / (6.0 + c[pl.ds(b, SLAB), :])
            return carry

        lax.fori_loop(2, 6, body, 0)

    each_x(second)

    for outer, y, inner in outer_sides:
        @pl.when(outer)
        def _():
            def run(x, kind):
                b = (x * 8 + y) * SLAB
                b = b if isinstance(b, int) else pl.multiple_of(b, 8)
                o = pl.ds((y * 8 + x) * SLAB, SLAB)
                total = slab(s, x, y) + zroll(slab(v, x, y, PAD)) + xsum(v, b + PAD, kind)
                total += slab(v, x, inner, PAD)
                w[o, :] = total / (6.0 + slab(c, x, y))
                o = pl.ds((inner * 8 + x) * SLAB, SLAB)
                w[o, :] = (w[o, :] + slab(v, x, y, PAD)) / (6.0 + slab(c, x, inner))

            each_x(run)

    end_row = lax.div(held - 1, LANES)
    for side, x, inner, at_row in ((0, 0, 1, 0), (1, 7, 6, end_row)):
        for i, (ref, at_x) in enumerate(((c, x), (c, inner), (u, x))):
            rows = pl.ds(at_x * step + at_row, 64, stride=OWN)
            ends[pl.ds((side * 3 + i) * 64, 64), :] = ref[rows, :]

    def keep(x, carry):
        def slab(ref, y):
            return ref[pl.ds(pl.multiple_of((x * 8 + y) * SLAB, 8), SLAB), :]

        for plane, value in enumerate(
            (
                slab(u, 0), slab(u, 7), slab(s, 0) + slab(u, 1), slab(s, 7) + slab(u, 6),
                slab(c, 0), slab(c, 1), slab(c, 7), slab(c, 6),
            )
        ):
            front[pl.ds(pl.multiple_of(PAD + (plane * 8 + x) * SLAB, 8), SLAB), :] = value
        return carry

    lax.fori_loop(0, 8, keep, 0)


def edge_kernel(
    held_ref, _, pack, ends, even_edge, odd_edge,
    new_pack, even_out, odd_out,
    edges, tail, head, sem,
):
    held = held_ref[0, 0]
    rank, ranks = lax.axis_index("curve"), lax.axis_size("curve")
    first_curve, last_curve = end_curves()
    take_zones(even_edge, odd_edge, edges.at[0], edges.at[1], sem, is_even("curve"))
    w = new_pack.at[pl.ds(PAD, CELLS * OWN)]
    lane, row = iota((64, LANES), 1), iota((64, LANES), 0)
    lone = jnp.logical_or(
        jnp.logical_and(row < 8, jnp.logical_not(first_curve)),
        jnp.logical_and(row >= 56, jnp.logical_not(last_curve)),
    )
    plain = jnp.logical_or(
        jnp.logical_and(row < 16, jnp.logical_not(first_curve)),
        jnp.logical_and(row >= 48, jnp.logical_not(last_curve)),
    )
    end_row, end_lane = lax.div(held - 1, LANES), lax.rem(held - 1, LANES)
    zero = jnp.zeros((8, LANES), F32)
    for side, x, inner, at_row, at_lane, there in (
        (0, 0, 1, 0, 0, rank > 0),
        (1, 7, 6, end_row, end_lane, rank < ranks - 1),
    ):
        a = spread(edges[side, 0:1, :])
        b = spread(edges[side, 1:2, :])
        coef, coef_inner, field = [ends[pl.ds((side * 3 + i) * 64, 64), :] for i in range(3)]
        hit = jnp.logical_and(lane == at_lane, jnp.logical_not(lone))
        more = jnp.where(hit, a[:64] / (6.0 + coef), 0.0)
        beyond = (a[64:] + field) / (6.0 + b[:64])
        total = jnp.where(jnp.logical_and(hit, there), beyond, 0.0) + up8(more) + down8(more)
        total += jnp.concatenate([zero, more[:-8]], 0) + jnp.concatenate([more[8:], zero], 0)
        total = total / jnp.where(plain, 1.0, 6.0 + coef)
        more = more / jnp.where(plain, 1.0, 6.0 + coef_inner)
        for at_x, value in ((x, total), (inner, more)):
            for y in range(8):
                o = pl.ds((y * 8 + at_x) * SLAB + at_row, 8, stride=OWN)
                w[o, :] = w[o, :] + value[8 * y : 8 * y + 8]

    place = tail_place(held)

    def body(i, carry):
        for k in range(8):
            at = pl.multiple_of((i * 8 + k) * SLAB, 8)
            load = lambda r, at=at: w[pl.ds(at + r, 8, stride=OWN), :]
            put_zones(load, tail, head, pl.multiple_of((i * 8 + k) * 8 * ZONE, 8), place)
        return carry

    lax.fori_loop(0, 8, body, 0)
    send_zones(tail, head, even_out, odd_out, sem, is_even("curve"))


class Window:
    def __init__(self, before, after):
        self.lane = iota((WIN, LANES), 1)
        self.row = iota((WIN, LANES), 0)
        j = self.row * LANES + self.lane
        down = lambda n: lax.shift_right_arithmetic(n, 7)
        self.own_row = down(-before)
        self.own_lane = jnp.bitwise_and(-before, LANES - 1)
        self.head_row = down(-AVG - after)
        self.head_lane = jnp.bitwise_and(-AVG - after, LANES - 1)
        self.tail_row = self.own_row + ZONE
        self.from_tail = j < before
        self.from_head = j >= AVG + after

    def take(self, ref, start, row, shift):
        a = ref[pl.ds(start + row, WIN), :]
        b = ref[pl.ds(start + row + 1, WIN), :]
        return pltpu.roll(
            jnp.where(self.lane >= shift, a, b), jnp.bitwise_and(LANES - shift, LANES - 1), 1
        )

    def __call__(self, own, own_at, tail, tail_at, head, head_at):
        mine = self.take(own, own_at, self.own_row, self.own_lane)
        prev = self.take(tail, tail_at, self.tail_row, self.own_lane)
        after = self.take(head, head_at, self.head_row, self.head_lane)
        return jnp.where(self.from_tail, prev, jnp.where(self.from_head, after, mine))


def drifts(held_ref, other_refs):
    rank, count = lax.axis_index("curve"), lax.axis_size("curve")
    held = held_ref[0, 0]
    total, before = held, -rank * AVG
    for i, ref in enumerate(other_refs):
        other = jnp.max(ref[...]).astype(jnp.int32)
        before += jnp.where(jnp.bitwise_and(rank, 1 << i) != 0, other, 0)
        total += other
    upper = jnp.bitwise_and(rank, 1 << len(other_refs)) != 0
    before += jnp.where(upper, count * AVG - total, 0)
    return before, before + held - AVG


def send_faces(low, high, even_out, odd_out, sem):
    even = is_even("grp")

    @pl.when(even)
    def _():
        run_copies([(high, even_out), (low, odd_out)], sem)

    @pl.when(jnp.logical_not(even))
    def _():
        run_copies([(low, even_out), (high, odd_out)], sem)


def take_faces(even_in, odd_in, low, high, sem):
    even = is_even("grp")

    @pl.when(even)
    def _():
        run_copies([(odd_in, low), (even_in, high)], sem)

    @pl.when(jnp.logical_not(even))
    def _():
        run_copies([(even_in, low), (odd_in, high)], sem)


def align_kernel(
    held_ref, before_refs, own, even_edge, odd_edge, even_1, odd_1, even_2, odd_2,
    even_out, odd_out, faces, sides,
    tail, head, edges, sem,
):
    before, after = drifts(held_ref, before_refs)
    even = is_even("curve")

    def one_side(zone, message, _):
        return [(message.at[pl.ds(0, PLANE)], to_plane(zone, plane_of(0, 0, 1)))]

    def both_sides(zone, _, message):
        return [(message.at[pl.ds(0, 2 * PLANE)], to_plane(zone, 0, 2))]

    by_parity((even_1, even_2), (odd_1, odd_2), tail, head, one_side, both_sides, sem)
    take_zones(even_edge, odd_edge, edges.at[0], edges.at[1], sem, even)
    here = Window(before, after)

    def body(k, carry):
        for z in range(8):
            i = k * 8 + z
            at = PAD + i * OWN
            zat = PAD + i * ZONE
            faces[pl.ds(pl.multiple_of(i * WIN, 8), WIN), :] = here(own, at, tail, zat, head, zat)
        return carry

    lax.fori_loop(0, 16, body, 0)
    lower = Window(before + 1, after + 1)
    upper = Window(before - 1, after - 1)
    j = here.row * LANES + here.lane
    for side, window, x, lost in (
        (0, lower, 7, jnp.logical_and(j == 0, before == HALF)),
        (1, upper, 0, jnp.logical_and(j == AVG - 1, after == -HALF)),
    ):
        beyond = spread(edges[side, 1:2, :])[64:]
        for plane in range(2):
            for z in range(8):
                i = (plane * 8 + x) * 8 + z
                at = PAD + i * OWN
                zat = PAD + i * ZONE
                value = window(own, at, tail, zat, head, zat)
                y = 56 * plane + z
                value = jnp.where(lost, beyond[y : y + 1], value)
                sides[pl.ds(((side * 2 + plane) * 8 + z) * WIN, WIN), :] = value
    half = 64 * WIN
    send_faces(faces.at[pl.ds(0, half)], faces.at[pl.ds(half, half)], even_out, odd_out, sem)


def each_x(run):
    run(0, 0)

    def mid(x, carry):
        run(x, 1)
        return carry

    lax.fori_loop(1, 7, mid, 0)
    run(7, 2)


def cell_rows(plane, x, z):
    at = ((plane * 8 + x) * 8 + z) * WIN
    return pl.ds(at if isinstance(at, int) else pl.multiple_of(at, 8), WIN)


def face_kernel(
    held_ref, before_refs, own, even_1, odd_1, even_2, odd_2,
    even_face, odd_face, faces, sides,
    even_out, odd_out, even_end, odd_end, new, below, inner,
    tail, head, near, q, ends, sem,
):
    before, after = drifts(held_ref, before_refs)
    even = is_even("curve")
    half = 64 * WIN

    def one_side(zone, message, _):
        return [
            (message.at[pl.ds(PLANE, PLANE)], to_plane(zone, plane_of(1, 2, 3))),
            (message.at[pl.ds(2 * PLANE, 2 * PLANE)], to_plane(zone, plane_of(2, 4, 6), 2)),
        ]

    def both_sides(zone, _, message):
        return [(message.at[pl.ds(2 * PLANE, 6 * PLANE)], to_plane(zone, 2 * PLANE, 6))]

    by_parity((even_1, even_2), (odd_1, odd_2), tail, head, one_side, both_sides, sem)
    take_faces(even_face, odd_face, near.at[pl.ds(0, half)], near.at[pl.ds(half, half)], sem)
    here = Window(before, after)

    def body(k, carry):
        for plane, ref, to, add in (
            (2, q, 0, 0.0),
            (3, q, 1, 0.0),
            (4, below, 0, 6.0),
            (6, below, 1, 6.0),
            (5, inner, 0, 6.0),
            (7, inner, 1, 6.0),
        ):
            for z in range(8):
                i = k * 8 + z
                at = PAD + (plane * 64 + i) * OWN
                zat = PAD + (plane * 64 + i) * ZONE
                value = here(own, at, tail, zat, head, zat)
                ref[pl.ds(pl.multiple_of((to * 64 + i) * WIN, 8), WIN), :] = value + add
        return carry

    lax.fori_loop(0, 8, body, 0)

    def run(x, kind):
        for plane in range(2):
            for z in range(8):
                here = cell_rows(plane, x, z)
                total = q[here, :] + near[here, :]
                if kind == 0:
                    total += sides[pl.ds((plane * 8 + z) * WIN, WIN), :]
                else:
                    total += faces[cell_rows(plane, x - 1, z), :]
                if kind == 2:
                    total += sides[pl.ds(((2 + plane) * 8 + z) * WIN, WIN), :]
                else:
                    total += faces[cell_rows(plane, x + 1, z), :]
                if z > 0:
                    total += faces[cell_rows(plane, x, z - 1), :]
                if z < 7:
                    total += faces[cell_rows(plane, x, z + 1), :]
                new[here, :] = total / below[here, :]

    each_x(run)
    for plane in range(2):
        for z in range(8):
            i = plane * 8 + z
            ends[0, i : i + 1, :] = new[pl.ds(((plane * 8 + 7) * 8 + z) * WIN + WIN - 1, 1), :]
            ends[1, i : i + 1, :] = new[pl.ds((plane * 64 + z) * WIN, 1), :]
    send_faces(new.at[pl.ds(0, half)], new.at[pl.ds(half, half)], even_out, odd_out, sem)
    send_zones(ends.at[0], ends.at[1], even_end, odd_end, sem, even)


def last_kernel(
    held_ref, before_refs, own, even_in, odd_in, even_face, odd_face, even_end, odd_end,
    new, below, inner,
    result,
    out, tail, head, near, ends, sem,
):
    before, after = drifts(held_ref, before_refs)
    even, even_curve = is_even("curve"), is_even("grp")
    half = 64 * WIN
    zone = pl.ds(PAD, 8 * 64 * ZONE)
    low, high = near.at[pl.ds(0, half)], near.at[pl.ds(half, half)]
    places = (tail.at[zone], head.at[zone], ends.at[0], ends.at[1], low, high)
    evens = (odd_in, even_in, odd_end, even_end)
    odds = (even_in, odd_in, even_end, odd_end)
    for flag, sources in ((even, evens), (jnp.logical_not(even), odds)):
        @pl.when(flag)
        def _():
            for copy in copies(list(zip(sources, places)), sem):
                copy.start()

    for flag, sources in (
        (even_curve, (odd_face, even_face)), (jnp.logical_not(even_curve), (even_face, odd_face))
    ):
        @pl.when(flag)
        def _():
            for i, source in enumerate(sources):
                pltpu.make_async_copy(source, places[4 + i], sem.at[4 + i]).start()

    for copy in copies(list(zip(evens + (even_face, odd_face), places)), sem):
        copy.wait()
    here = Window(before, after)
    lane, row = here.lane, here.row
    outer = end_curves()

    def get(y, x, z):
        i = (y * 8 + x) * 8 + z
        return here(own, PAD + i * OWN, tail, PAD + i * ZONE, head, PAD + i * ZONE)

    def put(x, y, z, value):
        at = ((x * 8 + y) * 8 + z) * WIN
        out[pl.ds(at if isinstance(at, int) else pl.multiple_of(at, 8), WIN), :] = value

    def left(plane, z):
        v = pltpu.roll(new[cell_rows(plane, 7, z), :], 1, 1)
        i = plane * 8 + z
        edge = pltpu.roll(jnp.broadcast_to(ends[0, i : i + 1, :], (WIN, LANES)), 1, 1)
        return jnp.where(lane == 0, jnp.where(row == 0, edge, pltpu.roll(v, 1, 0)), v)

    def right(plane, z):
        v = pltpu.roll(new[cell_rows(plane, 0, z), :], LANES - 1, 1)
        i = plane * 8 + z
        edge = pltpu.roll(jnp.broadcast_to(ends[1, i : i + 1, :], (WIN, LANES)), LANES - 1, 1)
        next_row = jnp.where(row == WIN - 1, edge, pltpu.roll(v, WIN - 1, 0))
        return jnp.where(lane == LANES - 1, next_row, v)

    def run(x, kind):
        for plane, y in ((0, 0), (1, 7)):
            for z in range(8):
                cell = cell_rows(plane, x, z)
                held = get(y, x, z)
                total = held + near[cell, :]
                total += left(plane, z) if kind == 0 else new[cell_rows(plane, x - 1, z), :]
                total += right(plane, z) if kind == 2 else new[cell_rows(plane, x + 1, z), :]
                if z > 0:
                    total += new[cell_rows(plane, x, z - 1), :]
                if z < 7:
                    total += new[cell_rows(plane, x, z + 1), :]
                put(x, y, z, jnp.where(outer[plane], held, total / below[cell, :]))
        for plane, y in ((0, 1), (1, 6)):
            for z in range(8):
                cell = cell_rows(plane, x, z)
                held = get(y, x, z)
                total = (held + new[cell, :]) / inner[cell, :]
                put(x, y, z, jnp.where(outer[plane], held, total))
        for y in range(2, 6):
            for z in range(8):
                put(x, y, z, get(y, x, z))
        store(x).start()

    def store(x):
        start = x * half
        rows = pl.ds(start if isinstance(start, int) else pl.multiple_of(start, 8), half)
        return pltpu.make_async_copy(out.at[rows], result.at[rows], sem.at[6 + x])

    each_x(run)
    for x in range(8):
        store(x).wait()


def swapped(value, axis, first, curves):
    count = lax.axis_size(axis)
    pairs = [(i, i + 1) for i in range(first, count - 1, 2)]
    pairs += [(b, a) for a, b in pairs]
    if curves is not None:
        all_curves = lax.axis_size("grp")
        pairs = [(a * all_curves + g, b * all_curves + g) for a, b in pairs for g in curves]
        axis = (axis, "grp")
    return lax.ppermute(value, axis, pairs)


def swaps(values, axis, curves=None):
    got = []
    for first, value in enumerate(values):
        got.append(swapped(value, axis, first, curves))
    return got


def add_kernel(a_ref, b_ref, sum_ref):
    sum_ref[...] = a_ref[...] + b_ref[...]


def counts_swapped(total):
    count, others = lax.axis_size("curve"), []
    vmem = pl.BlockSpec(memory_space=pltpu.VMEM)
    for i in range((count - 1).bit_length() - 1):
        if others:
            total = pl.pallas_call(
                add_kernel,
                out_shape=array(8, LANES),
                in_specs=[vmem, vmem],
                out_specs=vmem,
                compiler_params=pltpu.CompilerParams(vmem_limit_bytes=2**20),
            )(total, others[-1])
        pairs = [(a, a ^ 1 << i) for a in range(count) if a ^ 1 << i < count]
        others.append(lax.ppermute(total, "curve", pairs))
    return others


def array(*shape):
    return jax.ShapeDtypeStruct(shape, F32)


def call(kernel, outs, ins, scratch, limit, vmem_ins=(), vmem_outs=(), hbm_ins=(), us=2, aliases={}):
    (held,), others, *arrays = ins
    vmem = pl.BlockSpec(memory_space=pltpu.VMEM)
    specs = [SMEM] + [vmem] * len(others)
    specs += [
        vmem if i in vmem_ins else HBM if i in hbm_ins else ANY for i in range(len(arrays))
    ]

    def body(held_ref, *refs):
        kernel(held_ref, refs[: len(others)], *refs[len(others) :])

    return pl.pallas_call(
        body,
        out_shape=outs,
        in_specs=specs,
        out_specs=[vmem if i in vmem_outs else ANY for i in range(len(outs))],
        scratch_shapes=[pltpu.VMEM(shape, F32) for shape in scratch] + [pltpu.SemaphoreType.DMA((16,))],
        compiler_params=pltpu.CompilerParams(vmem_limit_bytes=limit * 2**20),
        cost_estimate=pl.CostEstimate(flops=us * 4_000_000, bytes_accessed=us * 10**6, transcendentals=0),
        input_output_aliases=aliases,
    )(held, *others, *arrays)


def local(state, coef, counts):
    state2 = state.reshape(2 * CELLS * OWN, LANES)
    coef2 = coef.reshape(CELLS * OWN, LANES)
    rows = CELLS * OWN
    zone = 64 * ZONE
    win = 64 * WIN

    message, edge = (8 * zone, LANES), (8, LANES)
    *outs, count = call(
        front_kernel,
        [array(*edge)] * 2 + [array(4 * zone, LANES)] * 2 + [array(*message)] * 2 + [array(8, LANES)],
        ((counts,), (), state2, coef2),
        [message, message, edge, edge],
        limit=6,
        vmem_ins=(0, 1),
        vmem_outs=(6,),
    )
    curves = lax.axis_size("grp")
    edges_in = swaps(outs[:2], "curve")
    others = counts_swapped(count)
    planes_in = swaps(outs[2:4], "curve", (0, curves - 1))
    planes_in += swaps(outs[4:], "curve", range(1, curves - 1))
    front, pack, ends = call(
        sweep_kernel,
        [array(rows + 2 * PAD, LANES)] * 2 + [array(6 * 64, LANES)],
        ((counts,), (), state2, coef2),
        [(rows + 2 * PAD, LANES)],
        limit=16,
        vmem_ins=(0, 1),
        vmem_outs=(0, 1, 2),
        us=6,
    )
    pack, *sweep_out = call(
        edge_kernel,
        [array(rows + 2 * PAD, LANES)] + [array(*message)] * 2,
        ((counts,), (), pack, ends, *edges_in),
        [(2, 8, LANES), message, message],
        limit=8,
        vmem_ins=(0, 1),
        vmem_outs=(0,),
        aliases={1: 0},
    )
    sweep_in = swaps(sweep_out, "curve")
    *near_out, faces, sides = call(
        align_kernel,
        [array(win, LANES)] * 2 + [array(2 * win, LANES), array(32 * WIN, LANES)],
        ((counts,), others, front, *edges_in, *planes_in),
        [(2 * zone + 2 * PAD, LANES), (2 * zone + 2 * PAD, LANES), (2, 8, LANES)],
        limit=8,
        vmem_ins=(0,),
        vmem_outs=(2, 3),
    )
    near_in = swaps(near_out, "grp")
    near_a, near_b, end_a, end_b, new, below, inner = call(
        face_kernel,
        [array(win, LANES)] * 2 + [array(16, LANES)] * 2 + [array(2 * win, LANES)] * 3,
        ((counts,), others, front, *planes_in, *near_in, faces, sides),
        [
            (8 * zone + 2 * PAD, LANES), (8 * zone + 2 * PAD, LANES),
            (2 * win, LANES), (2 * win, LANES), (2, 16, LANES),
        ],
        limit=8,
        vmem_ins=(0, 7, 8),
        vmem_outs=(4, 5, 6),
        us=3,
    )
    near_in = swaps((near_a, near_b), "grp")
    end_in = swaps((end_a, end_b), "curve")
    (out,) = call(
        last_kernel,
        [array(CELLS * WIN, LANES)],
        ((counts,), others, pack, *sweep_in, *near_in, *end_in, new, below, inner),
        [
            (CELLS * WIN, LANES), (8 * zone + 2 * PAD, LANES), (8 * zone + 2 * PAD, LANES),
            (2 * win, LANES), (2, 16, LANES),
        ],
        limit=12,
        vmem_ins=(0, 7, 8, 9),
        us=3,
    )
    return out.reshape(CELLS, 1, AVG)


def solution(mesh):
    placed = (P(None, None, "grp", "curve"), P(None, "grp", "curve"), P("grp", "curve"))

    return jax.shard_map(
        local, mesh=mesh, in_specs=placed, out_specs=P(None, "grp", "curve"), check_vma=False
    )
```

```python
import jax
import jax.numpy as jnp
from jax import lax
from jax.experimental import pallas as pl
from jax.experimental.pallas import tpu as pltpu
from jax.sharding import PartitionSpec as P


AVG = 1024
HALF = 256
CAP = 1536

LANES = 128
OWN = CAP // LANES
ZONE = HALF // LANES
WIN = AVG // LANES
SLAB = 8 * OWN
CELLS = 512
PAD = 16
PLANE = 64 * ZONE
F32 = jnp.float32
ANY = pl.BlockSpec(memory_space=pl.ANY)
HBM = pl.BlockSpec(memory_space=pltpu.HBM)
SMEM = pl.BlockSpec(memory_space=pltpu.SMEM)


def iota(shape, dim):
    return lax.broadcasted_iota(jnp.int32, shape, dim)


def copies(pairs, sems):
    return [pltpu.make_async_copy(a, b, sems.at[i]) for i, (a, b) in enumerate(pairs)]


def run_copies(pairs, sems):
    todo = copies(pairs, sems)
    for copy in todo:
        copy.start()
    for copy in todo:
        copy.wait()


def tail_place(held):
    first = held - HALF
    return lax.div(first, LANES), lax.rem(first, LANES)


def put_zones(load, tail, head, base, place):
    row, shift = place
    lane = iota((8, LANES), 1)
    for i in range(ZONE):
        head[pl.ds(base + i, 8, stride=ZONE), :] = load(i)
    rows = [load(jnp.minimum(row + i, OWN - 1)) for i in range(ZONE + 1)]
    back = lax.rem(LANES - shift, LANES)
    for i in range(ZONE):
        both = jnp.where(lane >= shift, rows[i], rows[i + 1])
        tail[pl.ds(base + i, 8, stride=ZONE), :] = pltpu.roll(both, back, 1)


def send_zones(tail, head, even_out, odd_out, sem, even):
    @pl.when(even)
    def _():
        run_copies([(tail, even_out), (head, odd_out)], sem)

    @pl.when(jnp.logical_not(even))
    def _():
        run_copies([(head, even_out), (tail, odd_out)], sem)


def take_zones(even_in, odd_in, tail, head, sem, even):
    @pl.when(even)
    def _():
        run_copies([(odd_in, tail), (even_in, head)], sem)

    @pl.when(jnp.logical_not(even))
    def _():
        run_copies([(even_in, tail), (odd_in, head)], sem)


def is_even(axis):
    return lax.rem(lax.axis_index(axis), 2) == 0


def up8(v):
    n = v.shape[0]
    z = lax.rem(iota(v.shape, 0), 8)
    return jnp.where(z < 7, pltpu.roll(v, n - 1, 0), 0.0)


def down8(v):
    z = lax.rem(iota(v.shape, 0), 8)
    return jnp.where(z > 0, pltpu.roll(v, 1, 0), 0.0)


def edge_rows(u_ref, s_ref, c_ref, outer, row, lane, extra_row):
    inner = 6 if outer == 7 else 1

    def at(ref, x, r):
        return ref[pl.ds(x * 8 * SLAB + r, 64, stride=OWN), :]

    u = at(u_ref, outer, row)
    side = at(s_ref, outer, row) + at(u_ref, inner, row) + up8(u) + down8(u)
    zero = jnp.zeros((8, LANES), F32)
    side += jnp.concatenate([zero, u[:-8]], 0) + jnp.concatenate([u[8:], zero], 0)
    parts = [(u, side), (at(c_ref, outer, row), at(u_ref, outer, extra_row))]
    back = lax.rem(LANES - lane, LANES)
    rows = []
    for pair in parts:
        square = pltpu.roll(jnp.concatenate(pair, 0), back, 1)
        rows.append(jnp.transpose(square)[0:1])
    return rows


def spread(packed):
    return jnp.transpose(jnp.broadcast_to(packed, (LANES, LANES)))


def end_curves():
    curve = lax.axis_index("grp")
    return curve == 0, curve == lax.axis_size("grp") - 1


def plane_of(inner, low, high):
    first, last = end_curves()
    plane = jnp.where(first, high, jnp.where(last, low, inner))
    return pl.multiple_of(plane * PLANE, 8)


def front_kernel(
    held_ref, _, state, coef,
    even_edge, odd_edge, even_1, odd_1, even_2, odd_2, count,
    tail, head, tail_edge, head_edge, sem,
):
    held = held_ref[0, 0]
    rows = CELLS * OWN
    u, c = state, coef
    s = state.at[pl.ds(rows, rows)]
    place = tail_place(held)
    even = is_even("curve")
    end = held - 1
    row, lane = lax.div(end, LANES), lax.rem(end, LANES)
    blank = jnp.zeros((6, LANES), F32)
    first = edge_rows(u, s, c, 0, 0, 0, ZONE)
    head_edge[...] = jnp.concatenate(first + [blank], 0)
    last = edge_rows(u, s, c, 7, row, lane, row - ZONE)
    tail_edge[...] = jnp.concatenate(last + [blank], 0)

    def at(ref, x, y):
        start = (x * 8 + y) * SLAB
        return lambda r: ref[pl.ds(start + r, 8, stride=OWN), :]

    def both(x, y, inner):
        return lambda r: at(u, x, inner)(r) + at(s, x, y)(r)

    for x in range(8):
        loads = [at(u, x, 0), at(u, x, 7), both(x, 0, 1), both(x, 7, 6)]
        loads += [at(c, x, y) for y in (0, 1, 7, 6)]
        for plane, load in enumerate(loads):
            put_zones(load, tail, head, (plane * 8 + x) * 8 * ZONE, place)

    count[...] = jnp.full((8, LANES), held, jnp.int32).astype(F32)

    def common(zone, edge, message):
        return [
            (zone.at[pl.ds(plane_of(0, 0, 1), PLANE)], message.at[pl.ds(0, PLANE)]),
            (zone.at[pl.ds(plane_of(1, 2, 3), PLANE)], message.at[pl.ds(PLANE, PLANE)]),
            (edge, message.at[pl.ds(2 * PLANE, 8)]),
        ]

    def one_side(zone, message, _):
        return [(zone.at[pl.ds(plane_of(2, 4, 6), 2 * PLANE)], message)]

    def both_sides(zone, _, message):
        return [(zone.at[pl.ds(2 * PLANE, 6 * PLANE)], message)]

    for flag, t, h, te, he in (
        (even, (even_1, even_2), (odd_1, odd_2), even_edge, odd_edge),
        (jnp.logical_not(even), (odd_1, odd_2), (even_1, even_2), odd_edge, even_edge),
    ):
        for kind, out in by_kind(one_side, both_sides):
            @pl.when(jnp.logical_and(flag, kind))
            def _():
                first = common(tail, tail_edge, te) + common(head, head_edge, he)
                run_copies(first + out(tail, *t) + out(head, *h), sem)


def by_kind(one_side, both_sides):
    first, last = end_curves()
    edge = jnp.logical_or(first, last)
    return (edge, one_side), (jnp.logical_not(edge), both_sides)


def by_parity(evens, odds, tail, head, one_side, both_sides, sem):
    even = is_even("curve")
    for flag, t, h in ((even, odds, evens), (jnp.logical_not(even), evens, odds)):
        for kind, to in by_kind(one_side, both_sides):
            @pl.when(jnp.logical_and(flag, kind))
            def _():
                run_copies(to(tail, *t) + to(head, *h), sem)


def take_edges(even_edge, odd_edge, edges, sem):
    rows = pl.ds(2 * PLANE, 8)
    take_zones(
        even_edge.at[rows], odd_edge.at[rows], edges.at[0], edges.at[1], sem, is_even("curve")
    )


def to_plane(zone, start, count=1):
    return zone.at[pl.ds(pl.multiple_of(PAD + start, 8), count * PLANE)]


def sweep_kernel(
    held_ref, _, state, coef,
    front, pack, ends,
    v, sem,
):
    held = held_ref[0, 0]
    first_curve, last_curve = end_curves()
    outer_sides = ((first_curve, 0, 1), (last_curve, 7, 6))
    u, c = state, coef
    s = state.at[pl.ds(CELLS * OWN, CELLS * OWN)]
    w = pack.at[pl.ds(PAD, CELLS * OWN)]
    row96 = iota((SLAB, LANES), 0)
    lane96 = iota((SLAB, LANES), 1)
    slot = lax.rem(row96, OWN) * LANES + lane96
    zlast, zfirst = row96 >= SLAB - OWN, row96 < OWN
    last_lane, first_lane = lane96 == LANES - 1, lane96 == 0
    starts = slot == 0
    finish = slot == held - 1

    def zsum(ref, b):
        up = jnp.where(zlast, 0.0, ref[pl.ds(b + OWN, SLAB), :])
        down = jnp.where(zfirst, 0.0, ref[pl.ds(b - OWN, SLAB), :])
        return up + down

    step = 8 * SLAB

    def left(ref, b):
        both = jnp.where(last_lane, ref[pl.ds(b - 1, SLAB), :], ref[pl.ds(b, SLAB), :])
        return jnp.where(starts, 0.0, pltpu.roll(both, 1, 1))

    def right(ref, b):
        both = jnp.where(first_lane, ref[pl.ds(b + 1, SLAB), :], ref[pl.ds(b, SLAB), :])
        return jnp.where(finish, 0.0, pltpu.roll(both, LANES - 1, 1))

    def xsum(ref, b, kind):
        if kind == 0:
            return left(ref, b + 7 * step) + ref[pl.ds(b + step, SLAB), :]
        if kind == 2:
            return ref[pl.ds(b - step, SLAB), :] + right(ref, b - 7 * step)
        return ref[pl.ds(b - step, SLAB), :] + ref[pl.ds(b + step, SLAB), :]

    def first(x, kind):
        def body(y, carry):
            b = (x * 8 + y) * SLAB
            if not isinstance(b, int):
                b = pl.multiple_of(b, 8)
            total = s[pl.ds(b, SLAB), :] + zsum(u, b) + xsum(u, b, kind)
            total += u[pl.ds(b - SLAB, SLAB), :] + u[pl.ds(b + SLAB, SLAB), :]
            v[pl.ds(b + PAD, SLAB), :] = total / (6.0 + c[pl.ds(b, SLAB), :])
            return carry

        lax.fori_loop(1, 7, body, 0)

    each_x(first)

    def slab(ref, x, y, off=0):
        b = off + (x * 8 + y) * SLAB
        return ref[pl.ds(b if isinstance(b, int) else pl.multiple_of(b, 8), SLAB), :]

    def zroll(value):
        up = jnp.where(zlast, 0.0, pltpu.roll(value, SLAB - OWN, 0))
        return up + jnp.where(zfirst, 0.0, pltpu.roll(value, OWN, 0))

    for outer, y, inner in outer_sides:
        @pl.when(outer)
        def _():
            def run(x, kind):
                b = (x * 8 + y) * SLAB
                b = b if isinstance(b, int) else pl.multiple_of(b, 8)
                total = slab(s, x, y) + zroll(slab(u, x, y)) + slab(u, x, inner) + xsum(u, b, kind)
                v[pl.ds(b + PAD, SLAB), :] = total / (6.0 + slab(c, x, y))

            each_x(run)

    def second(x, kind):
        def at(y):
            b = (x * 8 + y) * SLAB
            if not isinstance(b, int):
                b = pl.multiple_of(b, 8)
            return b, b + PAD

        def put(y, value):
            o = (y * 8 + x) * SLAB
            if not isinstance(o, int):
                o = pl.multiple_of(o, 8)
            w[pl.ds(o, SLAB), :] = value

        for y, inner in ((0, 1), (7, 6)):
            put(y, s[pl.ds(at(y)[0], SLAB), :] + v[pl.ds(at(inner)[1], SLAB), :])
        for y, inner in ((1, 2), (6, 5)):
            b, p = at(y)
            total = s[pl.ds(b, SLAB), :] + zsum(v, p) + xsum(v, p, kind)
            put(y, total + v[pl.ds(at(inner)[1], SLAB), :])

        def body(y, carry):
            b = (x * 8 + y) * SLAB
            b = b if isinstance(b, int) else pl.multiple_of(b, 8)
            p = b + PAD
            total = s[pl.ds(b, SLAB), :] + zsum(v, p) + xsum(v, p, kind)
            total += v[pl.ds(p - SLAB, SLAB), :] + v[pl.ds(p + SLAB, SLAB), :]
            o = pl.multiple_of((y * 8 + x) * SLAB, 8)
            w[pl.ds(o, SLAB), :] = total / (6.0 + c[pl.ds(b, SLAB), :])
            return carry

        lax.fori_loop(2, 6, body, 0)

    each_x(second)

    for outer, y, inner in outer_sides:
        @pl.when(outer)
        def _():
            def run(x, kind):
                b = (x * 8 + y) * SLAB
                b = b if isinstance(b, int) else pl.multiple_of(b, 8)
                o = pl.ds((y * 8 + x) * SLAB, SLAB)
                total = slab(s, x, y) + zroll(slab(v, x, y, PAD)) + xsum(v, b + PAD, kind)
                total += slab(v, x, inner, PAD)
                w[o, :] = total / (6.0 + slab(c, x, y))
                o = pl.ds((inner * 8 + x) * SLAB, SLAB)
                w[o, :] = (w[o, :] + slab(v, x, y, PAD)) / (6.0 + slab(c, x, inner))

            each_x(run)

    end_row = lax.div(held - 1, LANES)
    for side, x, inner, at_row in ((0, 0, 1, 0), (1, 7, 6, end_row)):
        for i, (ref, at_x) in enumerate(((c, x), (c, inner), (u, x))):
            rows = pl.ds(at_x * step + at_row, 64, stride=OWN)
            ends[pl.ds((side * 3 + i) * 64, 64), :] = ref[rows, :]

    def keep(x, carry):
        def slab(ref, y):
            return ref[pl.ds(pl.multiple_of((x * 8 + y) * SLAB, 8), SLAB), :]

        for plane, value in enumerate(
            (
                slab(u, 0), slab(u, 7), slab(s, 0) + slab(u, 1), slab(s, 7) + slab(u, 6),
                slab(c, 0), slab(c, 1), slab(c, 7), slab(c, 6),
            )
        ):
            front[pl.ds(pl.multiple_of(PAD + (plane * 8 + x) * SLAB, 8), SLAB), :] = value
        return carry

    lax.fori_loop(0, 8, keep, 0)


def edge_kernel(
    held_ref, _, pack, ends, even_edge, odd_edge,
    new_pack, even_out, odd_out,
    edges, tail, head, sem,
):
    held = held_ref[0, 0]
    rank, ranks = lax.axis_index("curve"), lax.axis_size("curve")
    first_curve, last_curve = end_curves()
    take_edges(even_edge, odd_edge, edges, sem)
    w = new_pack.at[pl.ds(PAD, CELLS * OWN)]
    lane, row = iota((64, LANES), 1), iota((64, LANES), 0)
    lone = jnp.logical_or(
        jnp.logical_and(row < 8, jnp.logical_not(first_curve)),
        jnp.logical_and(row >= 56, jnp.logical_not(last_curve)),
    )
    plain = jnp.logical_or(
        jnp.logical_and(row < 16, jnp.logical_not(first_curve)),
        jnp.logical_and(row >= 48, jnp.logical_not(last_curve)),
    )
    end_row, end_lane = lax.div(held - 1, LANES), lax.rem(held - 1, LANES)
    zero = jnp.zeros((8, LANES), F32)
    for side, x, inner, at_row, at_lane, there in (
        (0, 0, 1, 0, 0, rank > 0),
        (1, 7, 6, end_row, end_lane, rank < ranks - 1),
    ):
        a = spread(edges[side, 0:1, :])
        b = spread(edges[side, 1:2, :])
        coef, coef_inner, field = [ends[pl.ds((side * 3 + i) * 64, 64), :] for i in range(3)]
        hit = jnp.logical_and(lane == at_lane, jnp.logical_not(lone))
        more = jnp.where(hit, a[:64] / (6.0 + coef), 0.0)
        beyond = (a[64:] + field) / (6.0 + b[:64])
        total = jnp.where(jnp.logical_and(hit, there), beyond, 0.0) + up8(more) + down8(more)
        total += jnp.concatenate([zero, more[:-8]], 0) + jnp.concatenate([more[8:], zero], 0)
        total = total / jnp.where(plain, 1.0, 6.0 + coef)
        more = more / jnp.where(plain, 1.0, 6.0 + coef_inner)
        for at_x, value in ((x, total), (inner, more)):
            for y in range(8):
                o = pl.ds((y * 8 + at_x) * SLAB + at_row, 8, stride=OWN)
                w[o, :] = w[o, :] + value[8 * y : 8 * y + 8]

    place = tail_place(held)

    def body(i, carry):
        for k in range(8):
            at = pl.multiple_of((i * 8 + k) * SLAB, 8)
            load = lambda r, at=at: w[pl.ds(at + r, 8, stride=OWN), :]
            put_zones(load, tail, head, pl.multiple_of((i * 8 + k) * 8 * ZONE, 8), place)
        return carry

    lax.fori_loop(0, 8, body, 0)
    send_zones(tail, head, even_out, odd_out, sem, is_even("curve"))


class Window:
    def __init__(self, before, after):
        self.lane = iota((WIN, LANES), 1)
        self.row = iota((WIN, LANES), 0)
        j = self.row * LANES + self.lane
        down = lambda n: lax.shift_right_arithmetic(n, 7)
        self.own_row = down(-before)
        self.own_lane = jnp.bitwise_and(-before, LANES - 1)
        self.head_row = down(-AVG - after)
        self.head_lane = jnp.bitwise_and(-AVG - after, LANES - 1)
        self.tail_row = self.own_row + ZONE
        self.from_tail = j < before
        self.from_head = j >= AVG + after

    def take(self, ref, start, row, shift):
        a = ref[pl.ds(start + row, WIN), :]
        b = ref[pl.ds(start + row + 1, WIN), :]
        return pltpu.roll(
            jnp.where(self.lane >= shift, a, b), jnp.bitwise_and(LANES - shift, LANES - 1), 1
        )

    def __call__(self, own, own_at, tail, tail_at, head, head_at):
        mine = self.take(own, own_at, self.own_row, self.own_lane)
        prev = self.take(tail, tail_at, self.tail_row, self.own_lane)
        after = self.take(head, head_at, self.head_row, self.head_lane)
        return jnp.where(self.from_tail, prev, jnp.where(self.from_head, after, mine))


def drifts(held_ref, other_refs):
    rank, count = lax.axis_index("curve"), lax.axis_size("curve")
    held = held_ref[0, 0]
    total, before = held, -rank * AVG
    for i, ref in enumerate(other_refs):
        other = jnp.max(ref[...]).astype(jnp.int32)
        before += jnp.where(jnp.bitwise_and(rank, 1 << i) != 0, other, 0)
        total += other
    upper = jnp.bitwise_and(rank, 1 << len(other_refs)) != 0
    before += jnp.where(upper, count * AVG - total, 0)
    return before, before + held - AVG


def send_faces(low, high, even_out, odd_out, sem):
    even = is_even("grp")

    @pl.when(even)
    def _():
        run_copies([(high, even_out), (low, odd_out)], sem)

    @pl.when(jnp.logical_not(even))
    def _():
        run_copies([(low, even_out), (high, odd_out)], sem)


def take_faces(even_in, odd_in, low, high, sem):
    even = is_even("grp")

    @pl.when(even)
    def _():
        run_copies([(odd_in, low), (even_in, high)], sem)

    @pl.when(jnp.logical_not(even))
    def _():
        run_copies([(even_in, low), (odd_in, high)], sem)


def align_kernel(
    held_ref, before_refs, own, even_edge, odd_edge,
    even_out, odd_out, faces, sides,
    tail, head, edges, sem,
):
    before, after = drifts(held_ref, before_refs)
    even = is_even("curve")

    def one_side(zone, message):
        return [(message.at[pl.ds(0, PLANE)], to_plane(zone, plane_of(0, 0, 1)))]

    def both_sides(zone, message):
        return [(message.at[pl.ds(0, 2 * PLANE)], to_plane(zone, 0, 2))]

    by_parity((even_edge,), (odd_edge,), tail, head, one_side, both_sides, sem)
    take_edges(even_edge, odd_edge, edges, sem)
    here = Window(before, after)

    def body(k, carry):
        for z in range(8):
            i = k * 8 + z
            at = PAD + i * OWN
            zat = PAD + i * ZONE
            faces[pl.ds(pl.multiple_of(i * WIN, 8), WIN), :] = here(own, at, tail, zat, head, zat)
        return carry

    lax.fori_loop(0, 16, body, 0)
    lower = Window(before + 1, after + 1)
    upper = Window(before - 1, after - 1)
    j = here.row * LANES + here.lane
    for side, window, x, lost in (
        (0, lower, 7, jnp.logical_and(j == 0, before == HALF)),
        (1, upper, 0, jnp.logical_and(j == AVG - 1, after == -HALF)),
    ):
        beyond = spread(edges[side, 1:2, :])[64:]
        for plane in range(2):
            for z in range(8):
                i = (plane * 8 + x) * 8 + z
                at = PAD + i * OWN
                zat = PAD + i * ZONE
                value = window(own, at, tail, zat, head, zat)
                y = 56 * plane + z
                value = jnp.where(lost, beyond[y : y + 1], value)
                sides[pl.ds(((side * 2 + plane) * 8 + z) * WIN, WIN), :] = value
    half = 64 * WIN
    send_faces(faces.at[pl.ds(0, half)], faces.at[pl.ds(half, half)], even_out, odd_out, sem)


def each_x(run):
    run(0, 0)

    def mid(x, carry):
        run(x, 1)
        return carry

    lax.fori_loop(1, 7, mid, 0)
    run(7, 2)


def cell_rows(plane, x, z):
    at = ((plane * 8 + x) * 8 + z) * WIN
    return pl.ds(at if isinstance(at, int) else pl.multiple_of(at, 8), WIN)


def face_kernel(
    held_ref, before_refs, own, even_0, odd_0, even_1, odd_1, even_2, odd_2,
    even_face, odd_face, faces, sides,
    even_out, odd_out, even_end, odd_end, new, below, inner,
    tail, head, near, q, ends, sem,
):
    before, after = drifts(held_ref, before_refs)
    even = is_even("curve")
    half = 64 * WIN

    def one_side(zone, common, message, _):
        return [
            (common.at[pl.ds(PLANE, PLANE)], to_plane(zone, plane_of(1, 2, 3))),
            (message, to_plane(zone, plane_of(2, 4, 6), 2)),
        ]

    def both_sides(zone, _, __, message):
        return [(message, to_plane(zone, 2 * PLANE, 6))]

    by_parity((even_0, even_1, even_2), (odd_0, odd_1, odd_2), tail, head, one_side, both_sides, sem)
    take_faces(even_face, odd_face, near.at[pl.ds(0, half)], near.at[pl.ds(half, half)], sem)
    here = Window(before, after)

    def body(k, carry):
        for plane, ref, to, add in (
            (2, q, 0, 0.0),
            (3, q, 1, 0.0),
            (4, below, 0, 6.0),
            (6, below, 1, 6.0),
            (5, inner, 0, 6.0),
            (7, inner, 1, 6.0),
        ):
            for z in range(8):
                i = k * 8 + z
                at = PAD + (plane * 64 + i) * OWN
                zat = PAD + (plane * 64 + i) * ZONE
                value = here(own, at, tail, zat, head, zat)
                ref[pl.ds(pl.multiple_of((to * 64 + i) * WIN, 8), WIN), :] = value + add
        return carry

    lax.fori_loop(0, 8, body, 0)

    def run(x, kind):
        for plane in range(2):
            for z in range(8):
                here = cell_rows(plane, x, z)
                total = q[here, :] + near[here, :]
                if kind == 0:
                    total += sides[pl.ds((plane * 8 + z) * WIN, WIN), :]
                else:
                    total += faces[cell_rows(plane, x - 1, z), :]
                if kind == 2:
                    total += sides[pl.ds(((2 + plane) * 8 + z) * WIN, WIN), :]
                else:
                    total += faces[cell_rows(plane, x + 1, z), :]
                if z > 0:
                    total += faces[cell_rows(plane, x, z - 1), :]
                if z < 7:
                    total += faces[cell_rows(plane, x, z + 1), :]
                new[here, :] = total / below[here, :]

    each_x(run)
    for plane in range(2):
        for z in range(8):
            i = plane * 8 + z
            ends[0, i : i + 1, :] = new[pl.ds(((plane * 8 + 7) * 8 + z) * WIN + WIN - 1, 1), :]
            ends[1, i : i + 1, :] = new[pl.ds((plane * 64 + z) * WIN, 1), :]
    send_faces(new.at[pl.ds(0, half)], new.at[pl.ds(half, half)], even_out, odd_out, sem)
    send_zones(ends.at[0], ends.at[1], even_end, odd_end, sem, even)


def last_kernel(
    held_ref, before_refs, own, even_in, odd_in, even_face, odd_face, even_end, odd_end,
    new, below, inner,
    result,
    out, tail, head, near, ends, sem,
):
    before, after = drifts(held_ref, before_refs)
    even, even_curve = is_even("curve"), is_even("grp")
    half = 64 * WIN
    zone = pl.ds(PAD, 8 * 64 * ZONE)
    low, high = near.at[pl.ds(0, half)], near.at[pl.ds(half, half)]
    places = (tail.at[zone], head.at[zone], ends.at[0], ends.at[1], low, high)
    evens = (odd_in, even_in, odd_end, even_end)
    odds = (even_in, odd_in, even_end, odd_end)
    for flag, sources in ((even, evens), (jnp.logical_not(even), odds)):
        @pl.when(flag)
        def _():
            for copy in copies(list(zip(sources, places)), sem):
                copy.start()

    for flag, sources in (
        (even_curve, (odd_face, even_face)), (jnp.logical_not(even_curve), (even_face, odd_face))
    ):
        @pl.when(flag)
        def _():
            for i, source in enumerate(sources):
                pltpu.make_async_copy(source, places[4 + i], sem.at[4 + i]).start()

    for copy in copies(list(zip(evens + (even_face, odd_face), places)), sem):
        copy.wait()
    here = Window(before, after)
    lane, row = here.lane, here.row
    outer = end_curves()

    def get(y, x, z):
        i = (y * 8 + x) * 8 + z
        return here(own, PAD + i * OWN, tail, PAD + i * ZONE, head, PAD + i * ZONE)

    def put(x, y, z, value):
        at = ((x * 8 + y) * 8 + z) * WIN
        out[pl.ds(at if isinstance(at, int) else pl.multiple_of(at, 8), WIN), :] = value

    def left(plane, z):
        v = pltpu.roll(new[cell_rows(plane, 7, z), :], 1, 1)
        i = plane * 8 + z
        edge = pltpu.roll(jnp.broadcast_to(ends[0, i : i + 1, :], (WIN, LANES)), 1, 1)
        return jnp.where(lane == 0, jnp.where(row == 0, edge, pltpu.roll(v, 1, 0)), v)

    def right(plane, z):
        v = pltpu.roll(new[cell_rows(plane, 0, z), :], LANES - 1, 1)
        i = plane * 8 + z
        edge = pltpu.roll(jnp.broadcast_to(ends[1, i : i + 1, :], (WIN, LANES)), LANES - 1, 1)
        next_row = jnp.where(row == WIN - 1, edge, pltpu.roll(v, WIN - 1, 0))
        return jnp.where(lane == LANES - 1, next_row, v)

    def run(x, kind):
        for plane, y in ((0, 0), (1, 7)):
            for z in range(8):
                cell = cell_rows(plane, x, z)
                held = get(y, x, z)
                total = held + near[cell, :]
                total += left(plane, z) if kind == 0 else new[cell_rows(plane, x - 1, z), :]
                total += right(plane, z) if kind == 2 else new[cell_rows(plane, x + 1, z), :]
                if z > 0:
                    total += new[cell_rows(plane, x, z - 1), :]
                if z < 7:
                    total += new[cell_rows(plane, x, z + 1), :]
                put(x, y, z, jnp.where(outer[plane], held, total / below[cell, :]))
        for plane, y in ((0, 1), (1, 6)):
            for z in range(8):
                cell = cell_rows(plane, x, z)
                held = get(y, x, z)
                total = (held + new[cell, :]) / inner[cell, :]
                put(x, y, z, jnp.where(outer[plane], held, total))
        for y in range(2, 6):
            for z in range(8):
                put(x, y, z, get(y, x, z))
        store(x).start()

    def store(x):
        start = x * half
        rows = pl.ds(start if isinstance(start, int) else pl.multiple_of(start, 8), half)
        return pltpu.make_async_copy(out.at[rows], result.at[rows], sem.at[6 + x])

    each_x(run)
    for x in range(8):
        store(x).wait()


def swapped(value, axis, first, curves):
    count = lax.axis_size(axis)
    pairs = [(i, i + 1) for i in range(first, count - 1, 2)]
    pairs += [(b, a) for a, b in pairs]
    if curves is not None:
        all_curves = lax.axis_size("grp")
        pairs = [(a * all_curves + g, b * all_curves + g) for a, b in pairs for g in curves]
        axis = (axis, "grp")
    return lax.ppermute(value, axis, pairs)


def swaps(values, axis, curves=None):
    got = []
    for first, value in enumerate(values):
        got.append(swapped(value, axis, first, curves))
    return got


def add_kernel(a_ref, b_ref, sum_ref):
    sum_ref[...] = a_ref[...] + b_ref[...]


def counts_swapped(total):
    count, others = lax.axis_size("curve"), []
    vmem = pl.BlockSpec(memory_space=pltpu.VMEM)
    for i in range((count - 1).bit_length() - 1):
        if others:
            total = pl.pallas_call(
                add_kernel,
                out_shape=array(8, LANES),
                in_specs=[vmem, vmem],
                out_specs=vmem,
                compiler_params=pltpu.CompilerParams(vmem_limit_bytes=2**20),
            )(total, others[-1])
        pairs = [(a, a ^ 1 << i) for a in range(count) if a ^ 1 << i < count]
        others.append(lax.ppermute(total, "curve", pairs))
    return others


def array(*shape):
    return jax.ShapeDtypeStruct(shape, F32)


def call(kernel, outs, ins, scratch, limit, vmem_ins=(), vmem_outs=(), hbm_ins=(), us=2, aliases={}):
    (held,), others, *arrays = ins
    vmem = pl.BlockSpec(memory_space=pltpu.VMEM)
    specs = [SMEM] + [vmem] * len(others)
    specs += [
        vmem if i in vmem_ins else HBM if i in hbm_ins else ANY for i in range(len(arrays))
    ]

    def body(held_ref, *refs):
        kernel(held_ref, refs[: len(others)], *refs[len(others) :])

    return pl.pallas_call(
        body,
        out_shape=outs,
        in_specs=specs,
        out_specs=[vmem if i in vmem_outs else ANY for i in range(len(outs))],
        scratch_shapes=[pltpu.VMEM(shape, F32) for shape in scratch] + [pltpu.SemaphoreType.DMA((16,))],
        compiler_params=pltpu.CompilerParams(vmem_limit_bytes=limit * 2**20),
        cost_estimate=pl.CostEstimate(flops=us * 4_000_000, bytes_accessed=us * 10**6, transcendentals=0),
        input_output_aliases=aliases,
    )(held, *others, *arrays)


def local(state, coef, counts):
    state2 = state.reshape(2 * CELLS * OWN, LANES)
    coef2 = coef.reshape(CELLS * OWN, LANES)
    rows = CELLS * OWN
    zone = 64 * ZONE
    win = 64 * WIN

    message, edge = (8 * zone, LANES), (8, LANES)
    *outs, count = call(
        front_kernel,
        [array(2 * zone + 8, LANES)] * 2
        + [array(2 * zone, LANES)] * 2
        + [array(6 * zone, LANES)] * 2
        + [array(8, LANES)],
        ((counts,), (), state2, coef2),
        [message, message, edge, edge],
        limit=6,
        vmem_ins=(0, 1),
        vmem_outs=(6,),
    )
    curves = lax.axis_size("grp")
    edges_in = swaps(outs[:2], "curve")
    others = counts_swapped(count)
    planes_in = swaps(outs[2:4], "curve", (0, curves - 1))
    planes_in += swaps(outs[4:], "curve", range(1, curves - 1))
    front, pack, ends = call(
        sweep_kernel,
        [array(rows + 2 * PAD, LANES)] * 2 + [array(6 * 64, LANES)],
        ((counts,), (), state2, coef2),
        [(rows + 2 * PAD, LANES)],
        limit=16,
        vmem_ins=(0, 1),
        vmem_outs=(0, 1, 2),
        us=6,
    )
    pack, *sweep_out = call(
        edge_kernel,
        [array(rows + 2 * PAD, LANES)] + [array(*message)] * 2,
        ((counts,), (), pack, ends, *edges_in),
        [(2, 8, LANES), message, message],
        limit=8,
        vmem_ins=(0, 1),
        vmem_outs=(0,),
        aliases={1: 0},
    )
    sweep_in = swaps(sweep_out, "curve")
    *near_out, faces, sides = call(
        align_kernel,
        [array(win, LANES)] * 2 + [array(2 * win, LANES), array(32 * WIN, LANES)],
        ((counts,), others, front, *edges_in),
        [(2 * zone + 2 * PAD, LANES), (2 * zone + 2 * PAD, LANES), (2, 8, LANES)],
        limit=8,
        vmem_ins=(0,),
        vmem_outs=(2, 3),
    )
    near_in = swaps(near_out, "grp")
    near_a, near_b, end_a, end_b, new, below, inner = call(
        face_kernel,
        [array(win, LANES)] * 2 + [array(16, LANES)] * 2 + [array(2 * win, LANES)] * 3,
        ((counts,), others, front, *edges_in, *planes_in, *near_in, faces, sides),
        [
            (8 * zone + 2 * PAD, LANES), (8 * zone + 2 * PAD, LANES),
            (2 * win, LANES), (2 * win, LANES), (2, 16, LANES),
        ],
        limit=8,
        vmem_ins=(0, 9, 10),
        vmem_outs=(4, 5, 6),
        us=3,
    )
    near_in = swaps((near_a, near_b), "grp")
    end_in = swaps((end_a, end_b), "curve")
    (out,) = call(
        last_kernel,
        [array(CELLS * WIN, LANES)],
        ((counts,), others, pack, *sweep_in, *near_in, *end_in, new, below, inner),
        [
            (CELLS * WIN, LANES), (8 * zone + 2 * PAD, LANES), (8 * zone + 2 * PAD, LANES),
            (2 * win, LANES), (2, 16, LANES),
        ],
        limit=12,
        vmem_ins=(0, 7, 8, 9),
        us=3,
    )
    return out.reshape(CELLS, 1, AVG)


def solution(mesh):
    placed = (P(None, None, "grp", "curve"), P(None, "grp", "curve"), P("grp", "curve"))

    return jax.shard_map(
        local, mesh=mesh, in_specs=placed, out_specs=P(None, "grp", "curve"), check_vma=False
    )
```

```python
import jax
import jax.numpy as jnp
from jax import lax
from jax.experimental import pallas as pl
from jax.experimental.pallas import tpu as pltpu
from jax.sharding import PartitionSpec as P


AVG = 1024
HALF = 256
CAP = 1536

LANES = 128
OWN = CAP // LANES
ZONE = HALF // LANES
WIN = AVG // LANES
SLAB = 8 * OWN
CELLS = 512
PAD = 16
PLANE = 64 * ZONE
F32 = jnp.float32
ANY = pl.BlockSpec(memory_space=pl.ANY)
HBM = pl.BlockSpec(memory_space=pltpu.HBM)
SMEM = pl.BlockSpec(memory_space=pltpu.SMEM)


def iota(shape, dim):
    return lax.broadcasted_iota(jnp.int32, shape, dim)


def copies(pairs, sems):
    return [pltpu.make_async_copy(a, b, sems.at[i]) for i, (a, b) in enumerate(pairs)]


def run_copies(pairs, sems):
    todo = copies(pairs, sems)
    for copy in todo:
        copy.start()
    for copy in todo:
        copy.wait()


def tail_place(held):
    first = held - HALF
    return lax.div(first, LANES), lax.rem(first, LANES)


def put_zones(load, tail, head, base, place):
    row, shift = place
    lane = iota((8, LANES), 1)
    for i in range(ZONE):
        head[pl.ds(base + i, 8, stride=ZONE), :] = load(i)
    rows = [load(jnp.minimum(row + i, OWN - 1)) for i in range(ZONE + 1)]
    back = lax.rem(LANES - shift, LANES)
    for i in range(ZONE):
        both = jnp.where(lane >= shift, rows[i], rows[i + 1])
        tail[pl.ds(base + i, 8, stride=ZONE), :] = pltpu.roll(both, back, 1)


def send_zones(tail, head, even_out, odd_out, sem, even):
    @pl.when(even)
    def _():
        run_copies([(tail, even_out), (head, odd_out)], sem)

    @pl.when(jnp.logical_not(even))
    def _():
        run_copies([(head, even_out), (tail, odd_out)], sem)


def take_zones(even_in, odd_in, tail, head, sem, even):
    @pl.when(even)
    def _():
        run_copies([(odd_in, tail), (even_in, head)], sem)

    @pl.when(jnp.logical_not(even))
    def _():
        run_copies([(even_in, tail), (odd_in, head)], sem)


def is_even(axis):
    return lax.rem(lax.axis_index(axis), 2) == 0


def up8(v):
    n = v.shape[0]
    z = lax.rem(iota(v.shape, 0), 8)
    return jnp.where(z < 7, pltpu.roll(v, n - 1, 0), 0.0)


def down8(v):
    z = lax.rem(iota(v.shape, 0), 8)
    return jnp.where(z > 0, pltpu.roll(v, 1, 0), 0.0)


def edge_rows(u_ref, s_ref, c_ref, outer, row, lane, extra_row):
    inner = 6 if outer == 7 else 1

    def at(ref, x, r):
        return ref[pl.ds(x * 8 * SLAB + r, 64, stride=OWN), :]

    u = at(u_ref, outer, row)
    side = at(s_ref, outer, row) + at(u_ref, inner, row) + up8(u) + down8(u)
    zero = jnp.zeros((8, LANES), F32)
    side += jnp.concatenate([zero, u[:-8]], 0) + jnp.concatenate([u[8:], zero], 0)
    parts = [(u, side), (at(c_ref, outer, row), at(u_ref, outer, extra_row))]
    back = lax.rem(LANES - lane, LANES)
    rows = []
    for pair in parts:
        square = pltpu.roll(jnp.concatenate(pair, 0), back, 1)
        rows.append(jnp.transpose(square)[0:1])
    return rows


def spread(packed):
    return jnp.transpose(jnp.broadcast_to(packed, (LANES, LANES)))


def end_curves():
    curve = lax.axis_index("grp")
    return curve == 0, curve == lax.axis_size("grp") - 1


def plane_of(inner, low, high):
    first, last = end_curves()
    plane = jnp.where(first, high, jnp.where(last, low, inner))
    return pl.multiple_of(plane * PLANE, 8)


def front_kernel(
    held_ref, _, state, coef,
    even_edge, odd_edge, even_1, odd_1, even_2, odd_2, count,
    tail, head, tail_edge, head_edge, sem,
):
    held = held_ref[0, 0]
    rows = CELLS * OWN
    u, c = state, coef
    s = state.at[pl.ds(rows, rows)]
    place = tail_place(held)
    even = is_even("curve")
    end = held - 1
    row, lane = lax.div(end, LANES), lax.rem(end, LANES)
    blank = jnp.full((6, LANES), held, jnp.int32).astype(F32)
    first = edge_rows(u, s, c, 0, 0, 0, ZONE)
    head_edge[...] = jnp.concatenate(first + [blank], 0)
    last = edge_rows(u, s, c, 7, row, lane, row - ZONE)
    tail_edge[...] = jnp.concatenate(last + [blank], 0)

    def at(ref, x, y):
        start = (x * 8 + y) * SLAB
        return lambda r: ref[pl.ds(start + r, 8, stride=OWN), :]

    def both(x, y, inner):
        return lambda r: at(u, x, inner)(r) + at(s, x, y)(r)

    for x in range(8):
        loads = [at(u, x, 0), at(u, x, 7), both(x, 0, 1), both(x, 7, 6)]
        loads += [at(c, x, y) for y in (0, 1, 7, 6)]
        for plane, load in enumerate(loads):
            put_zones(load, tail, head, (plane * 8 + x) * 8 * ZONE, place)

    count[...] = jnp.full((8, LANES), held, jnp.int32).astype(F32)

    def common(zone, edge, message):
        return [
            (zone.at[pl.ds(plane_of(0, 0, 1), PLANE)], message.at[pl.ds(0, PLANE)]),
            (zone.at[pl.ds(plane_of(1, 2, 3), PLANE)], message.at[pl.ds(PLANE, PLANE)]),
            (edge, message.at[pl.ds(2 * PLANE, 8)]),
        ]

    def one_side(zone, message, _):
        return [(zone.at[pl.ds(plane_of(2, 4, 6), 2 * PLANE)], message)]

    def both_sides(zone, _, message):
        return [(zone.at[pl.ds(2 * PLANE, 6 * PLANE)], message)]

    for flag, t, h, te, he in (
        (even, (even_1, even_2), (odd_1, odd_2), even_edge, odd_edge),
        (jnp.logical_not(even), (odd_1, odd_2), (even_1, even_2), odd_edge, even_edge),
    ):
        for kind, out in by_kind(one_side, both_sides):
            @pl.when(jnp.logical_and(flag, kind))
            def _():
                first = common(tail, tail_edge, te) + common(head, head_edge, he)
                run_copies(first + out(tail, *t) + out(head, *h), sem)


def by_kind(one_side, both_sides):
    first, last = end_curves()
    edge = jnp.logical_or(first, last)
    return (edge, one_side), (jnp.logical_not(edge), both_sides)


def by_parity(evens, odds, tail, head, one_side, both_sides, sem):
    even = is_even("curve")
    for flag, t, h in ((even, odds, evens), (jnp.logical_not(even), evens, odds)):
        for kind, to in by_kind(one_side, both_sides):
            @pl.when(jnp.logical_and(flag, kind))
            def _():
                run_copies(to(tail, *t) + to(head, *h), sem)


def take_edges(even_edge, odd_edge, edges, sem):
    rows = pl.ds(2 * PLANE, 8)
    take_zones(
        even_edge.at[rows], odd_edge.at[rows], edges.at[0], edges.at[1], sem, is_even("curve")
    )


def to_plane(zone, start, count=1):
    return zone.at[pl.ds(pl.multiple_of(PAD + start, 8), count * PLANE)]


def sweep_kernel(
    held_ref, _, state, coef,
    front, pack, ends,
    v, sem,
):
    held = held_ref[0, 0]
    first_curve, last_curve = end_curves()
    outer_sides = ((first_curve, 0, 1), (last_curve, 7, 6))
    u, c = state, coef
    s = state.at[pl.ds(CELLS * OWN, CELLS * OWN)]
    w = pack.at[pl.ds(PAD, CELLS * OWN)]
    row96 = iota((SLAB, LANES), 0)
    lane96 = iota((SLAB, LANES), 1)
    slot = lax.rem(row96, OWN) * LANES + lane96
    zlast, zfirst = row96 >= SLAB - OWN, row96 < OWN
    last_lane, first_lane = lane96 == LANES - 1, lane96 == 0
    starts = slot == 0
    finish = slot == held - 1

    def zsum(ref, b):
        up = jnp.where(zlast, 0.0, ref[pl.ds(b + OWN, SLAB), :])
        down = jnp.where(zfirst, 0.0, ref[pl.ds(b - OWN, SLAB), :])
        return up + down

    step = 8 * SLAB

    def left(ref, b):
        both = jnp.where(last_lane, ref[pl.ds(b - 1, SLAB), :], ref[pl.ds(b, SLAB), :])
        return jnp.where(starts, 0.0, pltpu.roll(both, 1, 1))

    def right(ref, b):
        both = jnp.where(first_lane, ref[pl.ds(b + 1, SLAB), :], ref[pl.ds(b, SLAB), :])
        return jnp.where(finish, 0.0, pltpu.roll(both, LANES - 1, 1))

    def xsum(ref, b, kind):
        if kind == 0:
            return left(ref, b + 7 * step) + ref[pl.ds(b + step, SLAB), :]
        if kind == 2:
            return ref[pl.ds(b - step, SLAB), :] + right(ref, b - 7 * step)
        return ref[pl.ds(b - step, SLAB), :] + ref[pl.ds(b + step, SLAB), :]

    def first(x, kind):
        def body(y, carry):
            b = (x * 8 + y) * SLAB
            if not isinstance(b, int):
                b = pl.multiple_of(b, 8)
            total = s[pl.ds(b, SLAB), :] + zsum(u, b) + xsum(u, b, kind)
            total += u[pl.ds(b - SLAB, SLAB), :] + u[pl.ds(b + SLAB, SLAB), :]
            v[pl.ds(b + PAD, SLAB), :] = total / (6.0 + c[pl.ds(b, SLAB), :])
            return carry

        lax.fori_loop(1, 7, body, 0)

    each_x(first)

    def slab(ref, x, y, off=0):
        b = off + (x * 8 + y) * SLAB
        return ref[pl.ds(b if isinstance(b, int) else pl.multiple_of(b, 8), SLAB), :]

    def zroll(value):
        up = jnp.where(zlast, 0.0, pltpu.roll(value, SLAB - OWN, 0))
        return up + jnp.where(zfirst, 0.0, pltpu.roll(value, OWN, 0))

    for outer, y, inner in outer_sides:
        @pl.when(outer)
        def _():
            def run(x, kind):
                b = (x * 8 + y) * SLAB
                b = b if isinstance(b, int) else pl.multiple_of(b, 8)
                total = slab(s, x, y) + zroll(slab(u, x, y)) + slab(u, x, inner) + xsum(u, b, kind)
                v[pl.ds(b + PAD, SLAB), :] = total / (6.0 + slab(c, x, y))

            each_x(run)

    def second(x, kind):
        def at(y):
            b = (x * 8 + y) * SLAB
            if not isinstance(b, int):
                b = pl.multiple_of(b, 8)
            return b, b + PAD

        def put(y, value):
            o = (y * 8 + x) * SLAB
            if not isinstance(o, int):
                o = pl.multiple_of(o, 8)
            w[pl.ds(o, SLAB), :] = value

        for y, inner in ((0, 1), (7, 6)):
            put(y, s[pl.ds(at(y)[0], SLAB), :] + v[pl.ds(at(inner)[1], SLAB), :])
        for y, inner in ((1, 2), (6, 5)):
            b, p = at(y)
            total = s[pl.ds(b, SLAB), :] + zsum(v, p) + xsum(v, p, kind)
            put(y, total + v[pl.ds(at(inner)[1], SLAB), :])

        def body(y, carry):
            b = (x * 8 + y) * SLAB
            b = b if isinstance(b, int) else pl.multiple_of(b, 8)
            p = b + PAD
            total = s[pl.ds(b, SLAB), :] + zsum(v, p) + xsum(v, p, kind)
            total += v[pl.ds(p - SLAB, SLAB), :] + v[pl.ds(p + SLAB, SLAB), :]
            o = pl.multiple_of((y * 8 + x) * SLAB, 8)
            w[pl.ds(o, SLAB), :] = total / (6.0 + c[pl.ds(b, SLAB), :])
            return carry

        lax.fori_loop(2, 6, body, 0)

    each_x(second)

    for outer, y, inner in outer_sides:
        @pl.when(outer)
        def _():
            def run(x, kind):
                b = (x * 8 + y) * SLAB
                b = b if isinstance(b, int) else pl.multiple_of(b, 8)
                o = pl.ds((y * 8 + x) * SLAB, SLAB)
                total = slab(s, x, y) + zroll(slab(v, x, y, PAD)) + xsum(v, b + PAD, kind)
                total += slab(v, x, inner, PAD)
                w[o, :] = total / (6.0 + slab(c, x, y))
                o = pl.ds((inner * 8 + x) * SLAB, SLAB)
                w[o, :] = (w[o, :] + slab(v, x, y, PAD)) / (6.0 + slab(c, x, inner))

            each_x(run)

    end_row = lax.div(held - 1, LANES)
    for side, x, inner, at_row in ((0, 0, 1, 0), (1, 7, 6, end_row)):
        for i, (ref, at_x) in enumerate(((c, x), (c, inner), (u, x))):
            rows = pl.ds(at_x * step + at_row, 64, stride=OWN)
            ends[pl.ds((side * 3 + i) * 64, 64), :] = ref[rows, :]

    def keep(x, carry):
        def slab(ref, y):
            return ref[pl.ds(pl.multiple_of((x * 8 + y) * SLAB, 8), SLAB), :]

        for plane, value in enumerate(
            (
                slab(u, 0), slab(u, 7), slab(s, 0) + slab(u, 1), slab(s, 7) + slab(u, 6),
                slab(c, 0), slab(c, 1), slab(c, 7), slab(c, 6),
            )
        ):
            front[pl.ds(pl.multiple_of(PAD + (plane * 8 + x) * SLAB, 8), SLAB), :] = value
        return carry

    lax.fori_loop(0, 8, keep, 0)


def edge_kernel(
    held_ref, _, pack, ends, even_edge, odd_edge,
    new_pack, even_out, odd_out,
    edges, tail, head, sem,
):
    held = held_ref[0, 0]
    rank, ranks = lax.axis_index("curve"), lax.axis_size("curve")
    first_curve, last_curve = end_curves()
    take_edges(even_edge, odd_edge, edges, sem)
    w = new_pack.at[pl.ds(PAD, CELLS * OWN)]
    lane, row = iota((64, LANES), 1), iota((64, LANES), 0)
    lone = jnp.logical_or(
        jnp.logical_and(row < 8, jnp.logical_not(first_curve)),
        jnp.logical_and(row >= 56, jnp.logical_not(last_curve)),
    )
    plain = jnp.logical_or(
        jnp.logical_and(row < 16, jnp.logical_not(first_curve)),
        jnp.logical_and(row >= 48, jnp.logical_not(last_curve)),
    )
    end_row, end_lane = lax.div(held - 1, LANES), lax.rem(held - 1, LANES)
    zero = jnp.zeros((8, LANES), F32)
    for side, x, inner, at_row, at_lane, there in (
        (0, 0, 1, 0, 0, rank > 0),
        (1, 7, 6, end_row, end_lane, rank < ranks - 1),
    ):
        a = spread(edges[side, 0:1, :])
        b = spread(edges[side, 1:2, :])
        coef, coef_inner, field = [ends[pl.ds((side * 3 + i) * 64, 64), :] for i in range(3)]
        hit = jnp.logical_and(lane == at_lane, jnp.logical_not(lone))
        more = jnp.where(hit, a[:64] / (6.0 + coef), 0.0)
        beyond = (a[64:] + field) / (6.0 + b[:64])
        total = jnp.where(jnp.logical_and(hit, there), beyond, 0.0) + up8(more) + down8(more)
        total += jnp.concatenate([zero, more[:-8]], 0) + jnp.concatenate([more[8:], zero], 0)
        total = total / jnp.where(plain, 1.0, 6.0 + coef)
        more = more / jnp.where(plain, 1.0, 6.0 + coef_inner)
        for at_x, value in ((x, total), (inner, more)):
            for y in range(8):
                o = pl.ds((y * 8 + at_x) * SLAB + at_row, 8, stride=OWN)
                w[o, :] = w[o, :] + value[8 * y : 8 * y + 8]

    place = tail_place(held)

    def body(i, carry):
        for k in range(8):
            at = pl.multiple_of((i * 8 + k) * SLAB, 8)
            load = lambda r, at=at: w[pl.ds(at + r, 8, stride=OWN), :]
            put_zones(load, tail, head, pl.multiple_of((i * 8 + k) * 8 * ZONE, 8), place)
        return carry

    lax.fori_loop(0, 8, body, 0)
    send_zones(tail, head, even_out, odd_out, sem, is_even("curve"))


class Window:
    def __init__(self, before, after):
        self.lane = iota((WIN, LANES), 1)
        self.row = iota((WIN, LANES), 0)
        j = self.row * LANES + self.lane
        down = lambda n: lax.shift_right_arithmetic(n, 7)
        self.own_row = down(-before)
        self.own_lane = jnp.bitwise_and(-before, LANES - 1)
        self.head_row = down(-AVG - after)
        self.head_lane = jnp.bitwise_and(-AVG - after, LANES - 1)
        self.tail_row = self.own_row + ZONE
        self.from_tail = j < before
        self.from_head = j >= AVG + after

    def take(self, ref, start, row, shift):
        a = ref[pl.ds(start + row, WIN), :]
        b = ref[pl.ds(start + row + 1, WIN), :]
        return pltpu.roll(
            jnp.where(self.lane >= shift, a, b), jnp.bitwise_and(LANES - shift, LANES - 1), 1
        )

    def __call__(self, own, own_at, tail, tail_at, head, head_at):
        mine = self.take(own, own_at, self.own_row, self.own_lane)
        prev = self.take(tail, tail_at, self.tail_row, self.own_lane)
        after = self.take(head, head_at, self.head_row, self.head_lane)
        return jnp.where(self.from_tail, prev, jnp.where(self.from_head, after, mine))


def drifts(held_ref, other_refs):
    rank, count = lax.axis_index("curve"), lax.axis_size("curve")
    held = held_ref[0, 0]
    total, before = held, -rank * AVG
    for i, ref in enumerate(other_refs):
        other = jnp.max(ref[...]).astype(jnp.int32)
        before += jnp.where(jnp.bitwise_and(rank, 1 << i) != 0, other, 0)
        total += other
    upper = jnp.bitwise_and(rank, 1 << len(other_refs)) != 0
    before += jnp.where(upper, count * AVG - total, 0)
    return before, before + held - AVG


def send_faces(low, high, even_out, odd_out, sem):
    even = is_even("grp")

    @pl.when(even)
    def _():
        run_copies([(high, even_out), (low, odd_out)], sem)

    @pl.when(jnp.logical_not(even))
    def _():
        run_copies([(low, even_out), (high, odd_out)], sem)


def take_faces(even_in, odd_in, low, high, sem):
    even = is_even("grp")

    @pl.when(even)
    def _():
        run_copies([(odd_in, low), (even_in, high)], sem)

    @pl.when(jnp.logical_not(even))
    def _():
        run_copies([(even_in, low), (odd_in, high)], sem)


def align_kernel(
    held_ref, before_refs, own, even_edge, odd_edge,
    even_out, odd_out, faces, sides,
    tail, head, edges, sem,
):
    before, after = drifts(held_ref, before_refs)
    even = is_even("curve")

    def one_side(zone, message):
        return [(message.at[pl.ds(0, PLANE)], to_plane(zone, plane_of(0, 0, 1)))]

    def both_sides(zone, message):
        return [(message.at[pl.ds(0, 2 * PLANE)], to_plane(zone, 0, 2))]

    by_parity((even_edge,), (odd_edge,), tail, head, one_side, both_sides, sem)
    take_edges(even_edge, odd_edge, edges, sem)
    here = Window(before, after)

    def body(k, carry):
        for z in range(8):
            i = k * 8 + z
            at = PAD + i * OWN
            zat = PAD + i * ZONE
            faces[pl.ds(pl.multiple_of(i * WIN, 8), WIN), :] = here(own, at, tail, zat, head, zat)
        return carry

    lax.fori_loop(0, 16, body, 0)
    lower = Window(before + 1, after + 1)
    upper = Window(before - 1, after - 1)
    j = here.row * LANES + here.lane
    for side, window, x, lost in (
        (0, lower, 7, jnp.logical_and(j == 0, before == HALF)),
        (1, upper, 0, jnp.logical_and(j == AVG - 1, after == -HALF)),
    ):
        beyond = spread(edges[side, 1:2, :])[64:]
        for plane in range(2):
            for z in range(8):
                i = (plane * 8 + x) * 8 + z
                at = PAD + i * OWN
                zat = PAD + i * ZONE
                value = window(own, at, tail, zat, head, zat)
                y = 56 * plane + z
                value = jnp.where(lost, beyond[y : y + 1], value)
                sides[pl.ds(((side * 2 + plane) * 8 + z) * WIN, WIN), :] = value
    half = 64 * WIN
    send_faces(faces.at[pl.ds(0, half)], faces.at[pl.ds(half, half)], even_out, odd_out, sem)


def each_x(run):
    run(0, 0)

    def mid(x, carry):
        run(x, 1)
        return carry

    lax.fori_loop(1, 7, mid, 0)
    run(7, 2)


def cell_rows(plane, x, z):
    at = ((plane * 8 + x) * 8 + z) * WIN
    return pl.ds(at if isinstance(at, int) else pl.multiple_of(at, 8), WIN)


def face_kernel(
    held_ref, before_refs, own, even_0, odd_0, even_1, odd_1, even_2, odd_2,
    even_face, odd_face, faces, sides,
    even_out, odd_out, even_end, odd_end, new, below, inner,
    tail, head, near, q, ends, sem,
):
    before, after = drifts(held_ref, before_refs)
    even = is_even("curve")
    half = 64 * WIN

    def one_side(zone, common, message, _):
        return [
            (common.at[pl.ds(PLANE, PLANE)], to_plane(zone, plane_of(1, 2, 3))),
            (message, to_plane(zone, plane_of(2, 4, 6), 2)),
        ]

    def both_sides(zone, _, __, message):
        return [(message, to_plane(zone, 2 * PLANE, 6))]

    by_parity((even_0, even_1, even_2), (odd_0, odd_1, odd_2), tail, head, one_side, both_sides, sem)
    take_faces(even_face, odd_face, near.at[pl.ds(0, half)], near.at[pl.ds(half, half)], sem)
    here = Window(before, after)

    def body(k, carry):
        for plane, ref, to, add in (
            (2, q, 0, 0.0),
            (3, q, 1, 0.0),
            (4, below, 0, 6.0),
            (6, below, 1, 6.0),
            (5, inner, 0, 6.0),
            (7, inner, 1, 6.0),
        ):
            for z in range(8):
                i = k * 8 + z
                at = PAD + (plane * 64 + i) * OWN
                zat = PAD + (plane * 64 + i) * ZONE
                value = here(own, at, tail, zat, head, zat)
                ref[pl.ds(pl.multiple_of((to * 64 + i) * WIN, 8), WIN), :] = value + add
        return carry

    lax.fori_loop(0, 8, body, 0)

    def run(x, kind):
        for plane in range(2):
            for z in range(8):
                here = cell_rows(plane, x, z)
                total = q[here, :] + near[here, :]
                if kind == 0:
                    total += sides[pl.ds((plane * 8 + z) * WIN, WIN), :]
                else:
                    total += faces[cell_rows(plane, x - 1, z), :]
                if kind == 2:
                    total += sides[pl.ds(((2 + plane) * 8 + z) * WIN, WIN), :]
                else:
                    total += faces[cell_rows(plane, x + 1, z), :]
                if z > 0:
                    total += faces[cell_rows(plane, x, z - 1), :]
                if z < 7:
                    total += faces[cell_rows(plane, x, z + 1), :]
                new[here, :] = total / below[here, :]

    each_x(run)
    for plane in range(2):
        for z in range(8):
            i = plane * 8 + z
            ends[0, i : i + 1, :] = new[pl.ds(((plane * 8 + 7) * 8 + z) * WIN + WIN - 1, 1), :]
            ends[1, i : i + 1, :] = new[pl.ds((plane * 64 + z) * WIN, 1), :]
    send_faces(new.at[pl.ds(0, half)], new.at[pl.ds(half, half)], even_out, odd_out, sem)
    send_zones(ends.at[0], ends.at[1], even_end, odd_end, sem, even)


def last_kernel(
    held_ref, before_refs, own, even_in, odd_in, even_face, odd_face, even_end, odd_end,
    new, below, inner,
    result,
    out, tail, head, near, ends, sem,
):
    before, after = drifts(held_ref, before_refs)
    even, even_curve = is_even("curve"), is_even("grp")
    half = 64 * WIN
    zone = pl.ds(PAD, 8 * 64 * ZONE)
    low, high = near.at[pl.ds(0, half)], near.at[pl.ds(half, half)]
    places = (tail.at[zone], head.at[zone], ends.at[0], ends.at[1], low, high)
    evens = (odd_in, even_in, odd_end, even_end)
    odds = (even_in, odd_in, even_end, odd_end)
    for flag, sources in ((even, evens), (jnp.logical_not(even), odds)):
        @pl.when(flag)
        def _():
            for copy in copies(list(zip(sources, places)), sem):
                copy.start()

    for flag, sources in (
        (even_curve, (odd_face, even_face)), (jnp.logical_not(even_curve), (even_face, odd_face))
    ):
        @pl.when(flag)
        def _():
            for i, source in enumerate(sources):
                pltpu.make_async_copy(source, places[4 + i], sem.at[4 + i]).start()

    for copy in copies(list(zip(evens + (even_face, odd_face), places)), sem):
        copy.wait()
    here = Window(before, after)
    lane, row = here.lane, here.row
    outer = end_curves()

    def get(y, x, z):
        i = (y * 8 + x) * 8 + z
        return here(own, PAD + i * OWN, tail, PAD + i * ZONE, head, PAD + i * ZONE)

    def put(x, y, z, value):
        at = ((x * 8 + y) * 8 + z) * WIN
        out[pl.ds(at if isinstance(at, int) else pl.multiple_of(at, 8), WIN), :] = value

    def left(plane, z):
        v = pltpu.roll(new[cell_rows(plane, 7, z), :], 1, 1)
        i = plane * 8 + z
        edge = pltpu.roll(jnp.broadcast_to(ends[0, i : i + 1, :], (WIN, LANES)), 1, 1)
        return jnp.where(lane == 0, jnp.where(row == 0, edge, pltpu.roll(v, 1, 0)), v)

    def right(plane, z):
        v = pltpu.roll(new[cell_rows(plane, 0, z), :], LANES - 1, 1)
        i = plane * 8 + z
        edge = pltpu.roll(jnp.broadcast_to(ends[1, i : i + 1, :], (WIN, LANES)), LANES - 1, 1)
        next_row = jnp.where(row == WIN - 1, edge, pltpu.roll(v, WIN - 1, 0))
        return jnp.where(lane == LANES - 1, next_row, v)

    def run(x, kind):
        for plane, y in ((0, 0), (1, 7)):
            for z in range(8):
                cell = cell_rows(plane, x, z)
                held = get(y, x, z)
                total = held + near[cell, :]
                total += left(plane, z) if kind == 0 else new[cell_rows(plane, x - 1, z), :]
                total += right(plane, z) if kind == 2 else new[cell_rows(plane, x + 1, z), :]
                if z > 0:
                    total += new[cell_rows(plane, x, z - 1), :]
                if z < 7:
                    total += new[cell_rows(plane, x, z + 1), :]
                put(x, y, z, jnp.where(outer[plane], held, total / below[cell, :]))
        for plane, y in ((0, 1), (1, 6)):
            for z in range(8):
                cell = cell_rows(plane, x, z)
                held = get(y, x, z)
                total = (held + new[cell, :]) / inner[cell, :]
                put(x, y, z, jnp.where(outer[plane], held, total))
        for y in range(2, 6):
            for z in range(8):
                put(x, y, z, get(y, x, z))
        store(x).start()

    def store(x):
        start = x * half
        rows = pl.ds(start if isinstance(start, int) else pl.multiple_of(start, 8), half)
        return pltpu.make_async_copy(out.at[rows], result.at[rows], sem.at[6 + x])

    each_x(run)
    for x in range(8):
        store(x).wait()


def swapped(value, axis, first, curves):
    count = lax.axis_size(axis)
    pairs = [(i, i + 1) for i in range(first, count - 1, 2)]
    pairs += [(b, a) for a, b in pairs]
    if curves is not None:
        all_curves = lax.axis_size("grp")
        pairs = [(a * all_curves + g, b * all_curves + g) for a, b in pairs for g in curves]
        axis = (axis, "grp")
    return lax.ppermute(value, axis, pairs)


def swaps(values, axis, curves=None):
    got = []
    for first, value in enumerate(values):
        got.append(swapped(value, axis, first, curves))
    return got


def first_sum_kernel(count_ref, edge_ref, other_ref, sum_ref):
    other = jnp.broadcast_to(edge_ref[2 * PLANE + 2 : 2 * PLANE + 3, :], (8, LANES))
    other_ref[...] = other
    sum_ref[...] = count_ref[...] + other


def add_kernel(a_ref, b_ref, sum_ref):
    sum_ref[...] = a_ref[...] + b_ref[...]


def small_call(kernel, outs, *ins):
    vmem = pl.BlockSpec(memory_space=pltpu.VMEM)
    return pl.pallas_call(
        kernel,
        out_shape=[array(8, LANES)] * outs,
        in_specs=[vmem] * len(ins),
        out_specs=[vmem] * outs,
        compiler_params=pltpu.CompilerParams(vmem_limit_bytes=2**20),
    )(*ins)


def counts_swapped(count, edge):
    ranks, others = lax.axis_size("curve"), []
    for i in range((ranks - 1).bit_length() - 1):
        if i == 0:
            other, total = small_call(first_sum_kernel, 2, count, edge)
        else:
            pairs = [(a, a ^ 1 << i) for a in range(ranks) if a ^ 1 << i < ranks]
            other = lax.ppermute(total, "curve", pairs)
            if 2 << i < ranks // 2:
                (total,) = small_call(add_kernel, 1, total, other)
        others.append(other)
    return others


def array(*shape):
    return jax.ShapeDtypeStruct(shape, F32)


def call(kernel, outs, ins, scratch, limit, vmem_ins=(), vmem_outs=(), hbm_ins=(), us=2, aliases={}):
    (held,), others, *arrays = ins
    vmem = pl.BlockSpec(memory_space=pltpu.VMEM)
    specs = [SMEM] + [vmem] * len(others)
    specs += [
        vmem if i in vmem_ins else HBM if i in hbm_ins else ANY for i in range(len(arrays))
    ]

    def body(held_ref, *refs):
        kernel(held_ref, refs[: len(others)], *refs[len(others) :])

    return pl.pallas_call(
        body,
        out_shape=outs,
        in_specs=specs,
        out_specs=[vmem if i in vmem_outs else ANY for i in range(len(outs))],
        scratch_shapes=[pltpu.VMEM(shape, F32) for shape in scratch] + [pltpu.SemaphoreType.DMA((16,))],
        compiler_params=pltpu.CompilerParams(vmem_limit_bytes=limit * 2**20),
        cost_estimate=pl.CostEstimate(flops=us * 4_000_000, bytes_accessed=us * 10**6, transcendentals=0),
        input_output_aliases=aliases,
    )(held, *others, *arrays)


def local(state, coef, counts):
    state2 = state.reshape(2 * CELLS * OWN, LANES)
    coef2 = coef.reshape(CELLS * OWN, LANES)
    rows = CELLS * OWN
    zone = 64 * ZONE
    win = 64 * WIN

    message, edge = (8 * zone, LANES), (8, LANES)
    *outs, count = call(
        front_kernel,
        [array(2 * zone + 8, LANES)] * 2
        + [array(2 * zone, LANES)] * 2
        + [array(6 * zone, LANES)] * 2
        + [array(8, LANES)],
        ((counts,), (), state2, coef2),
        [message, message, edge, edge],
        limit=6,
        vmem_ins=(0, 1),
        vmem_outs=(6,),
    )
    curves = lax.axis_size("grp")
    edges_in = swaps(outs[:2], "curve")
    others = counts_swapped(count, edges_in[0])
    planes_in = swaps(outs[2:4], "curve", (0, curves - 1))
    planes_in += swaps(outs[4:], "curve", range(1, curves - 1))
    front, pack, ends = call(
        sweep_kernel,
        [array(rows + 2 * PAD, LANES)] * 2 + [array(6 * 64, LANES)],
        ((counts,), (), state2, coef2),
        [(rows + 2 * PAD, LANES)],
        limit=16,
        vmem_ins=(0, 1),
        vmem_outs=(0, 1, 2),
        us=6,
    )
    pack, *sweep_out = call(
        edge_kernel,
        [array(rows + 2 * PAD, LANES)] + [array(*message)] * 2,
        ((counts,), (), pack, ends, *edges_in),
        [(2, 8, LANES), message, message],
        limit=8,
        vmem_ins=(0, 1),
        vmem_outs=(0,),
        aliases={1: 0},
    )
    sweep_in = swaps(sweep_out, "curve")
    *near_out, faces, sides = call(
        align_kernel,
        [array(win, LANES)] * 2 + [array(2 * win, LANES), array(32 * WIN, LANES)],
        ((counts,), others, front, *edges_in),
        [(2 * zone + 2 * PAD, LANES), (2 * zone + 2 * PAD, LANES), (2, 8, LANES)],
        limit=8,
        vmem_ins=(0,),
        vmem_outs=(2, 3),
    )
    near_in = swaps(near_out, "grp")
    near_a, near_b, end_a, end_b, new, below, inner = call(
        face_kernel,
        [array(win, LANES)] * 2 + [array(16, LANES)] * 2 + [array(2 * win, LANES)] * 3,
        ((counts,), others, front, *edges_in, *planes_in, *near_in, faces, sides),
        [
            (8 * zone + 2 * PAD, LANES), (8 * zone + 2 * PAD, LANES),
            (2 * win, LANES), (2 * win, LANES), (2, 16, LANES),
        ],
        limit=8,
        vmem_ins=(0, 9, 10),
        vmem_outs=(4, 5, 6),
        us=3,
    )
    near_in = swaps((near_a, near_b), "grp")
    end_in = swaps((end_a, end_b), "curve")
    (out,) = call(
        last_kernel,
        [array(CELLS * WIN, LANES)],
        ((counts,), others, pack, *sweep_in, *near_in, *end_in, new, below, inner),
        [
            (CELLS * WIN, LANES), (8 * zone + 2 * PAD, LANES), (8 * zone + 2 * PAD, LANES),
            (2 * win, LANES), (2, 16, LANES),
        ],
        limit=12,
        vmem_ins=(0, 7, 8, 9),
        us=3,
    )
    return out.reshape(CELLS, 1, AVG)


def solution(mesh):
    placed = (P(None, None, "grp", "curve"), P(None, "grp", "curve"), P("grp", "curve"))

    return jax.shard_map(
        local, mesh=mesh, in_specs=placed, out_specs=P(None, "grp", "curve"), check_vma=False
    )
```
